256 devices in a mesh: grp: 8 (over y, core), dom: 32 (over z, x).
Axes of the slice: x: 4, y: 4, z: 8, core: 2. Of those that a mesh axis runs over, the one named last changes fastest.
Arguments:
- element_state: float32 [56, 9, 163840], P(None, None, ('grp', 'dom')), may hold values from -6 to 6
- stiffness: float32 [3, 56, 56], replicated, may hold values from -0.75 to 0.75
- flux_local: float32 [4, 56, 56], replicated, may hold values from -0.75 to 0.75
- flux_remote: float32 [4, 56, 56], replicated, may hold values from -0.75 to 0.75
- star_matrix: float32 [3, 9, 9, 163840], P(None, None, None, ('grp', 'dom')), may hold values from -0.18 to 0.18
- face_local: float32 [4, 9, 9, 163840], P(None, None, None, ('grp', 'dom')), may hold values from -0.15 to 0.15
- face_remote: float32 [4, 9, 9, 163840], P(None, None, None, ('grp', 'dom')), may hold values from -0.15 to 0.15
- energy_weight: float32 [9, 163840], P(None, ('grp', 'dom')), may hold values from 0.5 to 18
- face_neighbour: int32 [4, 163840], P(None, ('grp', 'dom')), may hold values from 0 to 1151, as said below
- element_count: int32 [256], P(('grp', 'dom')), may hold values from 160 to 640, as said below
- send_count: int32 [256, 8], P(('grp', 'dom')), may hold values from 0 to 64, as said below
- send_element: int32 [256, 8, 64], P(('grp', 'dom')), may hold values from 0 to 639, as said below
- receiver_element: int32 [4096], P(('grp', 'dom')), may hold values from 0 to 639, as said below
- receiver_slot: int32 [4096], P(('grp', 'dom')), may hold values from 0 to 511, as said below
- receiver_weight: float32 [56, 4096], P(None, ('grp', 'dom')), may hold values from -0.75 to 0.75
Outputs:
- new_state: float32 [56, 9, 163840], P(None, None, ('grp', 'dom'))
- energy: float32 [8, 3], P('grp')
- traces: float32 [3, 9, 4096], P(None, None, ('grp', 'dom'))
The draws below stay inside these ranges and needn't reach their ends.
Inputs may be any that keep to these rules, and one draw needn't show every extreme that they name: The first element_count[p] slots of a partition are active. In every slab 4 partitions in a row along dom (cyclically) hold 640 active elements; the others hold from 160 to 320. `send_count`: every partition has exactly 64 in one of its first 6 slots. `send_element`: names active elements of the sending partition. `face_neighbour`: values below 640 name active elements of the partition itself. `receiver_element`: names an active element of the owning partition. `receiver_slot`: within each slab a permutation of the 512 rows.
All inputs are finite; a program needn't handle non-finite values.
Results may differ from the reference program's by a relative error of at most 0.0001.
Values sent between devices are 32-bit elements; how exact they have to be, the bound alone decides.
A program may use at most 128 MiB of HBM per device.

```python
import jax
import jax.numpy as jnp
from jax import lax

BASIS_MODES = 56
QUANTITIES = 9
DIMENSIONS = 3
ELEM_FACES = 4
PEER_REACH = 3
TIME_STEPS = 3
HALO_CAP = 64
ELEM_PAD = 640
REC_DEV = 16
GROUPS = 8
GROUP_SIZE = 32
PARTITIONS = 256
PEER_SLOTS = 8
ELEMENTS = 163840
RECEIVERS = 4096


def partition_counts(key):
    base = jax.random.fold_in(key, 101)
    lighter = jax.random.randint(jax.random.fold_in(base, 1), (PARTITIONS,), ELEM_PAD // 4, ELEM_PAD // 2 + 1)
    window = jax.random.randint(jax.random.fold_in(base, 2), (GROUPS,), 0, GROUP_SIZE)
    numbers = jnp.arange(PARTITIONS, dtype=jnp.int32)
    position = (numbers % GROUP_SIZE - window[numbers // GROUP_SIZE]) % GROUP_SIZE
    return jnp.where(position < 4, ELEM_PAD, lighter).astype(jnp.int32)


def draw_element_count(key, part):
    return partition_counts(key)


def draw_send_count(key, part):
    counted = jax.random.randint(jax.random.fold_in(key, 201), (PARTITIONS, PEER_SLOTS), 0, HALO_CAP + 1)
    fullest = jax.random.randint(jax.random.fold_in(key, 202), (PARTITIONS, 1), 0, 2 * PEER_REACH)
    slots_row = jnp.arange(PEER_SLOTS, dtype=jnp.int32)[None, :]
    return jnp.where(slots_row == fullest, HALO_CAP, counted).astype(jnp.int32)


def draw_send_element(key, part):
    counts = partition_counts(key)
    return jax.random.randint(jax.random.fold_in(key, 301), (PARTITIONS, PEER_SLOTS, HALO_CAP), 0, counts[:, None, None]).astype(jnp.int32)


def draw_face_neighbour(key, part):
    counts = partition_counts(key)
    limits = jnp.repeat(counts, ELEM_PAD, total_repeat_length=ELEMENTS)[None, :]
    own_side = jax.random.randint(jax.random.fold_in(key, 401), (ELEM_FACES, ELEMENTS), 0, limits)
    far_side = ELEM_PAD + jax.random.randint(jax.random.fold_in(key, 402), (ELEM_FACES, ELEMENTS), 0, PEER_SLOTS * HALO_CAP)
    chosen = jax.random.randint(jax.random.fold_in(key, 403), (ELEM_FACES, ELEMENTS), 0, 4) == 0
    return jnp.where(chosen, far_side, own_side).astype(jnp.int32)


def draw_receiver_element(key, part):
    counts = partition_counts(key)
    limits = jnp.repeat(counts, REC_DEV, total_repeat_length=RECEIVERS)
    return jax.random.randint(jax.random.fold_in(key, 501), (RECEIVERS,), 0, limits).astype(jnp.int32)


def draw_receiver_slot(key, part):
    group_keys = jax.random.split(jax.random.fold_in(key, 601), GROUPS)
    orders = jax.vmap(lambda group_key: jax.random.permutation(group_key, GROUP_SIZE * REC_DEV))(group_keys)
    return orders.reshape(-1).astype(jnp.int32)


def draw_energy_weight(key, part):
    uniform_part = jax.random.uniform(jax.random.fold_in(key, 701), (QUANTITIES, ELEMENTS), jnp.float32)
    position = (jnp.arange(ELEMENTS, dtype=jnp.int32) // ELEM_PAD % GROUP_SIZE).astype(jnp.float32)
    rising = 1.0 + 2.0 * position / (GROUP_SIZE - 1)
    return (jnp.exp(jnp.log(0.5) + uniform_part * jnp.log(4.0)) * rising).astype(jnp.float32)


def level_of(key, shape, cuts, low, largest):
    gain = 1.0
    for axis_at, blocks in cuts:
        draws = jax.random.uniform(jax.random.fold_in(jax.random.fold_in(key, 6), axis_at), (blocks,), jnp.float32, low / len(cuts), largest / len(cuts))
        gain = gain * jnp.repeat(jnp.exp(draws), shape[axis_at] // blocks).reshape((-1,) + (1,) * (len(shape) - 1 - axis_at))
    return gain


def normal_values(rng, shape, deviation, bound, cuts=(), kind=jnp.bfloat16):
    result = deviation * jax.random.normal(rng, shape, jnp.float32)
    if cuts:
        result = result * level_of(rng, shape, cuts, -0.22, 0.18)
    return jnp.clip(result, -bound, bound).astype(kind)


def setup_inputs(seed: int = 0) -> dict:
    arg_keys = jax.random.split(jax.random.key(seed), 16)
    element_state = normal_values(arg_keys[0], (BASIS_MODES, QUANTITIES, ELEMENTS), 1.0, 6.0, ((2, 256),), jnp.float32)
    stiffness = normal_values(arg_keys[1], (DIMENSIONS, BASIS_MODES, BASIS_MODES), BASIS_MODES ** -0.5, 0.75, (), jnp.float32)
    flux_local = normal_values(arg_keys[2], (ELEM_FACES, BASIS_MODES, BASIS_MODES), BASIS_MODES ** -0.5, 0.75, (), jnp.float32)
    flux_remote = normal_values(arg_keys[3], (ELEM_FACES, BASIS_MODES, BASIS_MODES), BASIS_MODES ** -0.5, 0.75, (), jnp.float32)
    star_matrix = normal_values(arg_keys[4], (DIMENSIONS, QUANTITIES, QUANTITIES, ELEMENTS), 0.03, 0.18, ((3, 256),), jnp.float32)
    face_local = normal_values(arg_keys[5], (ELEM_FACES, QUANTITIES, QUANTITIES, ELEMENTS), 0.025, 0.15, ((3, 256),), jnp.float32)
    face_remote = normal_values(arg_keys[6], (ELEM_FACES, QUANTITIES, QUANTITIES, ELEMENTS), 0.025, 0.15, ((3, 256),), jnp.float32)
    energy_weight = draw_energy_weight(jax.random.fold_in(arg_keys[15], 71), 0)
    face_neighbour = draw_face_neighbour(jax.random.fold_in(arg_keys[15], 71), 0)
    element_count = draw_element_count(jax.random.fold_in(arg_keys[15], 71), 0)
    send_count = draw_send_count(jax.random.fold_in(arg_keys[15], 71), 0)
    send_element = draw_send_element(jax.random.fold_in(arg_keys[15], 71), 0)
    receiver_element = draw_receiver_element(jax.random.fold_in(arg_keys[15], 71), 0)
    receiver_slot = draw_receiver_slot(jax.random.fold_in(arg_keys[15], 71), 0)
    receiver_weight = normal_values(arg_keys[14], (BASIS_MODES, RECEIVERS), BASIS_MODES ** -0.5, 0.75, ((1, 256),), jnp.float32)
    return dict(element_state=element_state, stiffness=stiffness, flux_local=flux_local, flux_remote=flux_remote, star_matrix=star_matrix, face_local=face_local, face_remote=face_remote, energy_weight=energy_weight, face_neighbour=face_neighbour, element_count=element_count, send_count=send_count, send_element=send_element, receiver_element=receiver_element, receiver_slot=receiver_slot, receiver_weight=receiver_weight)


highest = lax.Precision.HIGHEST


def modal(matrix, field):
    flat = field.reshape(field.shape[0], -1)
    product = jnp.dot(matrix, flat, precision=highest, preferred_element_type=jnp.float32)
    return product.reshape((matrix.shape[0],) + field.shape[1:])


def quantity_map(matrices, field):
    return jnp.einsum("pqe,bqe->bpe", matrices, field, precision=highest)


def per_partition(array):
    shaped = array.reshape(array.shape[:-1] + (PARTITIONS, ELEM_PAD))
    return jnp.moveaxis(shaped, -2, 0)


def slot_offset(slot_number):
    if slot_number < PEER_REACH:
        return slot_number + 1
    if slot_number < 2 * PEER_REACH:
        return PEER_REACH - 1 - slot_number
    if slot_number == 2 * PEER_REACH:
        return 1
    return -1


def reference(element_state, stiffness, flux_local, flux_remote, star_matrix, face_local, face_remote, energy_weight, face_neighbour, element_count, send_count, send_element, receiver_element, receiver_slot, receiver_weight):
    fields = per_partition(element_state)
    stars = per_partition(star_matrix)
    local_faces = per_partition(face_local)
    remote_faces = per_partition(face_remote)
    weights = per_partition(energy_weight)
    neighbours = per_partition(face_neighbour)
    receiver_rows = jnp.moveaxis(receiver_weight.reshape(BASIS_MODES, PARTITIONS, REC_DEV), 1, 0)
    receiver_cells = receiver_element.reshape(PARTITIONS, REC_DEV)
    numbers = jnp.arange(PARTITIONS, dtype=jnp.int32)
    group_of = numbers // GROUP_SIZE
    place_of = numbers % GROUP_SIZE
    source_list = []
    present_list = []
    for slot_number in range(PEER_SLOTS):
        offset = slot_offset(slot_number)
        if slot_number < 2 * PEER_REACH:
            source_list.append(group_of * GROUP_SIZE + (place_of - offset) % GROUP_SIZE)
            present_list.append(jnp.ones((PARTITIONS,), dtype=bool))
        else:
            other = group_of - offset
            present_list.append((other >= 0) & (other < GROUPS))
            source_list.append(jnp.clip(other, 0, GROUPS - 1) * GROUP_SIZE + place_of)
    sources = jnp.stack(source_list, 1).astype(jnp.int32)
    present = jnp.stack(present_list, 1)
    live_mask = jnp.arange(ELEM_PAD, dtype=jnp.int32)[None, :] < element_count[:, None]
    slot_live = jnp.arange(HALO_CAP, dtype=jnp.int32)[None, None, :] < send_count[:, :, None]
    denominator = GROUP_SIZE * ELEM_PAD * BASIS_MODES * QUANTITIES
    global_slot = ((jnp.arange(RECEIVERS, dtype=jnp.int32) // (GROUP_SIZE * REC_DEV)) * (GROUP_SIZE * REC_DEV) + receiver_slot).astype(jnp.int32)

    def pack(field, elements, live):
        taken = jnp.take(field, elements, axis=2)
        return jnp.where(live[None, None], taken, jnp.float32(0.0))

    def advance(fields):
        messages = jax.vmap(pack)(fields, send_element, slot_live)

        def update_one(items):
            field, star_here, local_here, remote_here, neighbour_here, source_here, present_here, live_here = items
            pieces = []
            for slot_number in range(PEER_SLOTS):
                sent = lax.dynamic_index_in_dim(messages, source_here[slot_number], 0, keepdims=False)[:, :, slot_number, :]
                pieces.append(jnp.where(present_here[slot_number], sent, jnp.float32(0.0)))
            halo = jnp.stack(pieces, 2).reshape(BASIS_MODES, QUANTITIES, PEER_SLOTS * HALO_CAP)
            extended = jnp.concatenate([field, halo], 2)
            change = jnp.zeros(field.shape, jnp.float32)
            for dimension in range(DIMENSIONS):
                change = change + quantity_map(star_here[dimension], modal(stiffness[dimension], field))
            for face_number in range(ELEM_FACES):
                change = change - quantity_map(local_here[face_number], modal(flux_local[face_number], field))
                nearby = jnp.take(extended, neighbour_here[face_number], axis=2)
                change = change - quantity_map(remote_here[face_number], modal(flux_remote[face_number], nearby))
            return jnp.where(live_here[None, None, :], field + change, field)

        return lax.map(update_one, (fields, stars, local_faces, remote_faces, neighbours, sources, present, live_mask))

    energies = []
    tables = []
    for time_step in range(TIME_STEPS):
        fields = advance(fields)
        squares = jnp.sum(fields * fields, axis=1)
        terms = 0.5 * jnp.sum(jnp.where(live_mask[:, None, :], weights * squares, jnp.float32(0.0)), axis=(1, 2))
        energies.append(terms.reshape(GROUPS, GROUP_SIZE).sum(1) / denominator)

        def sample(field, elements, rows_here):
            return jnp.einsum("br,bqr->qr", rows_here, jnp.take(field, elements, axis=2), precision=highest)

        values = jax.vmap(sample)(fields, receiver_cells, receiver_rows)
        flat = jnp.moveaxis(values, 0, 1).reshape(QUANTITIES, RECEIVERS)
        tables.append(jnp.zeros((QUANTITIES, RECEIVERS), jnp.float32).at[:, global_slot].set(flat))
    new_state = jnp.moveaxis(fields, 0, 2).reshape(BASIS_MODES, QUANTITIES, ELEMENTS)
    return new_state, jnp.stack(energies, 1), jnp.stack(tables, 0)
```

```python
import jax
import jax.numpy as jnp
from jax import lax
from jax.experimental import pallas as pl
from jax.experimental.pallas import tpu as pltpu
from jax.sharding import PartitionSpec as P

STEPS = 3
REACH = 3
GRP_DOM = ("grp", "dom")
MESH = pl.DeviceIdType.MESH
f32 = jnp.float32
bf16 = jnp.bfloat16
highest = lax.Precision.HIGHEST
LANES = 128
CHUNKS = 4
ROWS_LHS = 176
TN = (((0,), (0,)), ((), ()))
NT = (((1,), (1,)), ((), ()))


def offset_of(slot):
    return slot + 1 if slot < REACH else REACH - 1 - slot


def split(value):
    hi = value.astype(bf16)
    return hi, (value - hi.astype(f32)).astype(bf16)


def lane_block(number):
    return pl.ds(pl.multiple_of(number * LANES, LANES), LANES)


def make_kernel(groups, places, elems, cap):
    slots = 2 * REACH + 2
    blocks = elems // LANES
    sent = slots * cap
    receivers = 16

    def kernel(
        state_ref, stiff_ref, flux_ref, fluxr_ref, star_ref, face_ref, facer_ref,
        weight_ref, live_ref, number_ref, recw_ref,
        x_ref, energy_ref, trace_ref,
        y_ref, v_ref, part_ref, xt_ref, send_buf, halo_ref, hb_ref, own_ref, nb_ref, vr_ref,
        pick_ref, pack_ref, af_ref, a_ref, rf_ref, ra_ref, rb_ref,
        en_ref, rec_ref, table_ref, msg_ref, all_ref,
        send_sem, recv_sem, last_send, last_recv,
    ):
        g = lax.axis_index("grp")
        d = lax.axis_index("dom")

        for t in range(STEPS):
            halo_ref[t, 2 * REACH * cap :, :] = jnp.zeros((2 * cap, CHUNKS * LANES), f32)
        barrier = pltpu.get_barrier_semaphore()

        def greet(k, carry):
            peer = lax.rem(d + k, places)
            pl.semaphore_signal(barrier, inc=1, device_id=(g, peer), device_id_type=MESH)
            return carry

        lax.fori_loop(1, places, greet, 0)

        @pl.when(g < groups - 1)
        def _():
            pl.semaphore_signal(barrier, inc=1, device_id=(g + 1, d), device_id_type=MESH)

        @pl.when(g > 0)
        def _():
            pl.semaphore_signal(barrier, inc=1, device_id=(g - 1, d), device_id_type=MESH)

        for q in range(9):
            x_ref[q] = state_ref[q]

        lane = lax.broadcasted_iota(jnp.int32, (LANES, LANES), 1).astype(f32)

        def column(number):
            return jnp.broadcast_to(number_ref[number], (LANES, LANES)).T

        def hot(names, tile):
            return jnp.maximum(1.0 - jnp.abs(names - (lane + float(tile * LANES))), 0.0).astype(bf16)

        def pack_rows(i, carry):
            names = column(4 * blocks + i)
            at = pl.ds(pl.multiple_of(i * LANES, LANES), LANES)
            for tile in range(blocks):
                pack_ref[at, tile * LANES : (tile + 1) * LANES] = hot(names, tile)
            return carry

        lax.fori_loop(0, sent // LANES + 1, pack_rows, 0)

        def to_rows():
            def body(block, carry):
                at = lane_block(block)
                for j in range(CHUNKS):
                    size = min(16, 56 - 16 * j)
                    pieces = [x_ref[2 * j, :, at], x_ref[2 * j + 1, :, at], x_ref[8, pl.ds(16 * j, size), at]]
                    if size < 16:
                        pieces.append(jnp.zeros((16 - size, LANES), f32))
                    hi, lo = split(jnp.concatenate(pieces, axis=0).T)
                    xt_ref[at, 2 * j * LANES : (2 * j + 1) * LANES] = hi
                    xt_ref[at, (2 * j + 1) * LANES : (2 * j + 2) * LANES] = lo
                return carry

            lax.fori_loop(0, blocks, body, 0)

        def pack(first, count):
            for j in range(CHUNKS):
                taken = jnp.dot(
                    pack_ref[first : first + count, :],
                    xt_ref[:, 2 * j * LANES : (2 * j + 2) * LANES],
                    preferred_element_type=f32,
                )
                whole = taken[:, :LANES] + taken[:, LANES:]
                if first == 0:
                    send_buf[:, j * LANES : (j + 1) * LANES] = whole[:sent]
                    rec_ref[:, j * LANES : (j + 1) * LANES] = whole[sent:]
                else:
                    rec_ref[:, j * LANES : (j + 1) * LANES] = whole

        def copies(t):
            made = []
            for slot in range(slots):
                if slot < 2 * REACH:
                    target = (g, lax.rem(d + offset_of(slot) + places, places))
                else:
                    target = (g + (1 if slot == 2 * REACH else -1), d)
                made.append(
                    pltpu.make_async_remote_copy(
                        src_ref=send_buf.at[pl.ds(slot * cap, cap)],
                        dst_ref=halo_ref.at[t, pl.ds(slot * cap, cap)],
                        send_sem=send_sem.at[slot],
                        recv_sem=recv_sem.at[t, slot],
                        device_id=target,
                        device_id_type=MESH,
                    )
                )
            return made

        def trace(t):
            at = lax.broadcasted_iota(jnp.int32, (CHUNKS * LANES, LANES), 0)
            inside = at % LANES
            quantity = jnp.where(inside < 56, at // LANES * 2, jnp.where(inside < 112, at // LANES * 2 + 1, 8))
            out = lax.broadcasted_iota(jnp.int32, (CHUNKS * LANES, LANES), 1)
            placed = jnp.where(out == 9 * t + quantity, 1.0, 0.0).astype(f32)
            table_ref[...] += jnp.dot(
                rec_ref[...] * recw_ref[...], placed, precision=highest, preferred_element_type=f32
            )

        to_rows()
        table_ref[...] = jnp.zeros_like(table_ref)
        en_ref[...] = jnp.zeros_like(en_ref)

        def step(t, carry):
            pack(0, sent + receivers)

            @pl.when(t == 0)
            def _():
                waits = places - 1 + jnp.where(g > 0, 1, 0) + jnp.where(g < groups - 1, 1, 0)
                pl.semaphore_wait(barrier, waits)

            moves = copies(t)
            for slot in range(2 * REACH):
                moves[slot].start()

            @pl.when(g < groups - 1)
            def _():
                moves[6].start()

            @pl.when(g > 0)
            def _():
                moves[7].start()

            @pl.when(t == 0)
            def _():
                af_ref[...] = jnp.zeros_like(af_ref)
                for m in range(7):
                    matrix = stiff_ref[m] if m < 3 else -flux_ref[m - 3]
                    for part in range(4):
                        af_ref[pl.ds(56 * m, 56), pl.ds(64 * part, 56)] = matrix
                whole = af_ref[...]
                rounded = whole.astype(bf16).astype(f32)
                part = lax.broadcasted_iota(jnp.int32, whole.shape, 1) // 64
                a_ref[...] = jnp.where(part % 2 == 0, rounded, whole - rounded).astype(bf16)
                for f in range(4):
                    matrix = -fluxr_ref[f]
                    for j in range(CHUNKS):
                        rf_ref[...] = jnp.zeros_like(rf_ref)
                        rf_ref[pl.ds(0, 56), pl.ds(0, 56)] = matrix
                        rf_ref[pl.ds(56, 56), pl.ds(56, 56)] = matrix
                        size = min(16, 56 - 16 * j)
                        rf_ref[pl.ds(112, 56), pl.ds(112, size)] = matrix[:, 16 * j : 16 * j + size]
                        hi, lo = split(rf_ref[...])
                        ra_ref[f, j] = jnp.concatenate([hi, hi], axis=1)
                        rb_ref[f, j] = jnp.concatenate([lo, lo], axis=1)

                def face_rows(i, carry):
                    names = column(i)
                    f = i // blocks
                    at = pl.ds(pl.multiple_of(i % blocks * LANES, LANES), LANES)
                    for tile in range(blocks + sent // LANES):
                        pick_ref[f, at, tile * LANES : (tile + 1) * LANES] = hot(names, tile)
                    return carry

                lax.fori_loop(0, 4 * blocks, face_rows, 0)

            @pl.when(t > 0)
            def _():
                trace(t - 1)

            def modal(q, carry):
                pad = jnp.zeros((8, elems), f32)
                value = jnp.concatenate([x_ref[q], pad], axis=0)
                hi, lo = split(value)
                y_ref[0:64, :] = hi
                y_ref[64:128, :] = hi
                y_ref[128:192, :] = lo
                y_ref[192:256, :] = lo
                v_ref[q] = jnp.dot(a_ref[...], y_ref[...], preferred_element_type=f32)
                return carry

            lax.fori_loop(0, 9, modal, 0)

            def local_map(number, carry):
                block = number // 3
                first = (number % 3) * 3
                at = lane_block(block)
                total = [jnp.zeros((56, LANES), f32) for _ in range(3)]
                for m in range(7):
                    maps, n = (star_ref, m) if m < 3 else (face_ref, m - 3)
                    for q in range(9):
                        term = v_ref[q, pl.ds(56 * m, 56), at]
                        for i in range(3):
                            total[i] = total[i] + maps[first + i, q, pl.ds(n, 1), at] * term
                for i in range(3):
                    part_ref[first + i, :, at] = total[i]
                return carry

            lax.fori_loop(0, blocks * 3, local_map, 0)

            def own(f, carry):
                for j in range(CHUNKS):
                    own_ref[f, j] = jnp.dot(
                        pick_ref[f, :, :elems],
                        xt_ref[:, 2 * j * LANES : (2 * j + 2) * LANES],
                        preferred_element_type=f32,
                    ).astype(bf16)
                return carry

            lax.fori_loop(0, 4, own, 0)

            for slot in range(2 * REACH):
                moves[slot].wait_recv()

            @pl.when(g > 0)
            def _():
                moves[6].wait_recv()

            @pl.when(g < groups - 1)
            def _():
                moves[7].wait_recv()

            for j in range(CHUNKS):
                hi, lo = split(halo_ref[t, :, j * LANES : (j + 1) * LANES])
                hb_ref[:, 2 * j * LANES : (2 * j + 1) * LANES] = hi
                hb_ref[:, (2 * j + 1) * LANES : (2 * j + 2) * LANES] = lo

            def remote(f, carry):
                for j in range(CHUNKS):
                    far = jnp.dot(
                        pick_ref[f, :, elems:],
                        hb_ref[:, 2 * j * LANES : (2 * j + 2) * LANES],
                        preferred_element_type=f32,
                    ).astype(bf16)
                    nb_ref[...] = own_ref[f, j] + far
                    near = nb_ref[...]
                    both = lax.dot_general(ra_ref[f, j], near, NT, preferred_element_type=f32)
                    both = both + lax.dot_general(rb_ref[f, j], near, NT, preferred_element_type=f32)
                    vr_ref[f, 2 * j] = both[0:56]
                    vr_ref[f, 2 * j + 1] = both[56:112]
                    if j == 0:
                        vr_ref[f, 8] = both[112:168]
                    else:
                        vr_ref[f, 8] += both[112:168]
                return carry

            lax.fori_loop(0, 4, remote, 0)

            def remote_map(number, energy):
                block = number // 3
                first = (number % 3) * 3
                at = lane_block(block)
                live = live_ref[0, :, at]
                total = [part_ref[first + i, :, at] for i in range(3)]
                for f in range(4):
                    for q in range(9):
                        term = vr_ref[f, q, :, at]
                        for i in range(3):
                            total[i] = total[i] + facer_ref[first + i, q, pl.ds(f, 1), at] * term
                for i in range(3):
                    new = x_ref[first + i, :, at] + live * total[i]
                    x_ref[first + i, :, at] = new
                    squares = jnp.sum(new * new, axis=0, keepdims=True)
                    energy = energy + weight_ref[first + i, :, at] * squares
                return energy

            energy = lax.fori_loop(0, blocks * 3, remote_map, jnp.zeros((1, LANES), f32))
            sub = lax.broadcasted_iota(jnp.int32, (8, LANES), 0)
            en_ref[...] += jnp.where(sub == t, energy, 0.0)
            to_rows()

            for slot in range(2 * REACH):
                moves[slot].wait_send()

            @pl.when(g < groups - 1)
            def _():
                moves[6].wait_send()

            @pl.when(g > 0)
            def _():
                moves[7].wait_send()

            return carry

        lax.fori_loop(0, STEPS, step, 0)
        pack(sent, receivers)
        trace(STEPS - 1)

        row = lax.broadcasted_iota(jnp.int32, (receivers, LANES), 0)
        col = lax.broadcasted_iota(jnp.int32, (receivers, LANES), 1)
        rows = column(4 * blocks + sent // LANES + 1)[:receivers]
        sums = jnp.sum(en_ref[...], axis=1, keepdims=True)
        table = table_ref[...] + jnp.where(col == 27, rows, 0.0)
        for t in range(STEPS):
            table = table + jnp.where((col == 28 + t) & (row == 0), sums[t : t + 1], 0.0)
        half = receivers // 2
        msg_ref[...] = table[:half] + pltpu.roll(table[half:], 64, 1)

        def last(k):
            return pltpu.make_async_remote_copy(
                src_ref=msg_ref,
                dst_ref=all_ref.at[d],
                send_sem=last_send.at[k],
                recv_sem=last_recv.at[k],
                device_id=(g, lax.rem(d + k, places)),
                device_id_type=MESH,
            )

        def arrival(k):
            return pltpu.make_async_remote_copy(
                src_ref=msg_ref,
                dst_ref=all_ref.at[lax.rem(d + places - k, places)],
                send_sem=last_send.at[k],
                recv_sem=last_recv.at[k],
                device_id=(g, lax.rem(d + k, places)),
                device_id_type=MESH,
            )

        def start_last(k, carry):
            last(k).start()
            return carry

        def end_last(k, carry):
            arrival(k).wait_recv()
            last(k).wait_send()
            return carry

        lax.fori_loop(1, places, start_last, 0)
        all_ref[d] = msg_ref[...]
        lax.fori_loop(1, places, end_last, 0)

        arrived = all_ref[...].reshape(places * half, LANES)
        energy_ref[...] = jnp.broadcast_to(jnp.sum(arrived, axis=0, keepdims=True), energy_ref.shape)
        mine = lax.broadcasted_iota(jnp.int32, (places * half, LANES), 1).astype(f32)
        mine = mine + (d * receivers).astype(f32)
        keep = lax.broadcasted_iota(jnp.int32, (places * half, LANES), 1) < receivers
        result = jnp.zeros(trace_ref.shape, f32)
        for part in range(2):
            names = jnp.broadcast_to(arrived[:, 64 * part + 27 : 64 * part + 28], (places * half, LANES))
            chosen = jnp.maximum(1.0 - jnp.abs(names - mine), 0.0)
            chosen = jnp.where(keep, chosen, 0.0)
            picked = lax.dot_general(arrived, chosen, TN, precision=highest, preferred_element_type=f32)
            result = result + picked[64 * part : 64 * part + 32]
        trace_ref[...] = result

    return kernel


def per_device(groups, places):
    def run(
        element_state, stiffness, flux_local, flux_remote, star_matrix, face_local, face_remote,
        energy_weight, face_neighbour, element_count, send_count, send_element,
        receiver_element, receiver_slot, receiver_weight,
    ):
        basis, quantities, elems = element_state.shape
        slots, cap = send_element.shape[1:]
        sent = slots * cap
        receivers = receiver_slot.shape[0]
        turned = receiver_weight.T
        tail = jnp.pad(turned, ((0, 0), (0, 8))).reshape(receivers, CHUNKS, 16)
        pair = jnp.broadcast_to(turned[:, None, :], (receivers, CHUNKS, basis))
        recw = jnp.concatenate([pair, pair, tail], axis=2).reshape(receivers, CHUNKS * LANES)
        live = (jnp.arange(elems) < element_count[0]).astype(f32)
        weight = (energy_weight * live[None])[:, None, :]
        filled = jnp.arange(cap)[None, :] < send_count[0][:, None]
        wanted = jnp.where(filled, send_element[0], -1)
        fill = LANES - receivers
        numbers = jnp.concatenate(
            [
                face_neighbour.reshape(-1, LANES),
                wanted.reshape(-1, LANES),
                jnp.pad(receiver_element, (0, fill), constant_values=-1)[None],
                jnp.pad(receiver_slot, (0, fill), constant_values=-1)[None],
            ],
            axis=0,
        ).astype(f32)[:, None, :]

        vmem = pl.BlockSpec(memory_space=pltpu.VMEM)
        wide = CHUNKS * LANES
        faces = 4
        state, energy, table = pl.pallas_call(
            make_kernel(groups, places, elems, cap),
            out_shape=(
                jax.ShapeDtypeStruct((quantities, basis, elems), f32),
                jax.ShapeDtypeStruct((8, LANES), f32),
                jax.ShapeDtypeStruct((32, LANES), f32),
            ),
            in_specs=[vmem] * 11,
            out_specs=(vmem, vmem, vmem),
            scratch_shapes=[
                pltpu.VMEM((256, elems), bf16),
                pltpu.VMEM((9, 400, elems), f32),
                pltpu.VMEM((9, 56, elems), f32),
                pltpu.VMEM((elems, 2 * wide), bf16),
                pltpu.VMEM((sent, wide), f32),
                pltpu.VMEM((STEPS, sent, wide), f32),
                pltpu.VMEM((sent, 2 * wide), bf16),
                pltpu.VMEM((faces, CHUNKS, elems, 2 * LANES), bf16),
                pltpu.VMEM((elems, 2 * LANES), bf16),
                pltpu.VMEM((faces, 9, 56, elems), f32),
                pltpu.VMEM((faces, elems, elems + sent), bf16),
                pltpu.VMEM((sent + LANES, elems), bf16),
                pltpu.VMEM((400, 256), f32),
                pltpu.VMEM((400, 256), bf16),
                pltpu.VMEM((ROWS_LHS, LANES), f32),
                pltpu.VMEM((faces, CHUNKS, ROWS_LHS, 2 * LANES), bf16),
                pltpu.VMEM((faces, CHUNKS, ROWS_LHS, 2 * LANES), bf16),
                pltpu.VMEM((8, LANES), f32),
                pltpu.VMEM((receivers, wide), f32),
                pltpu.VMEM((receivers, LANES), f32),
                pltpu.VMEM((receivers // 2, LANES), f32),
                pltpu.VMEM((places, receivers // 2, LANES), f32),
                pltpu.SemaphoreType.DMA((slots,)),
                pltpu.SemaphoreType.DMA((STEPS, slots)),
                pltpu.SemaphoreType.DMA((places,)),
                pltpu.SemaphoreType.DMA((places,)),
            ],
            compiler_params=pltpu.CompilerParams(
                collective_id=0, has_side_effects=True, vmem_limit_bytes=60 * 1024 * 1024
            ),
        )(
            element_state.transpose(1, 0, 2), stiffness, flux_local, flux_remote,
            star_matrix.transpose(1, 2, 0, 3), face_local.transpose(1, 2, 0, 3),
            face_remote.transpose(1, 2, 0, 3),
            weight, live[None, None], numbers, recw,
        )
        total = energy[:1, 28 : 28 + STEPS] * 0.5 / float(places * elems * basis * quantities)
        traces = table[: STEPS * quantities, :receivers].reshape(STEPS, quantities, receivers)
        return state.transpose(1, 0, 2), total, traces

    return run


def solution(mesh):
    return jax.shard_map(
        per_device(mesh.shape["grp"], mesh.shape["dom"]),
        mesh=mesh,
        in_specs=(
            P(None, None, GRP_DOM), P(), P(), P(),
            P(None, None, None, GRP_DOM), P(None, None, None, GRP_DOM), P(None, None, None, GRP_DOM),
            P(None, GRP_DOM), P(None, GRP_DOM), P(GRP_DOM), P(GRP_DOM, None), P(GRP_DOM, None, None),
            P(GRP_DOM), P(GRP_DOM), P(None, GRP_DOM),
        ),
        out_specs=(P(None, None, GRP_DOM), P("grp", None), P(None, None, GRP_DOM)),
        check_vma=False,
    )
```

```python
import jax
import jax.numpy as jnp
from jax import lax
from jax.experimental import pallas as pl
from jax.experimental.pallas import tpu as pltpu
from jax.sharding import PartitionSpec as P

STEPS = 3
REACH = 3
GRP_DOM = ("grp", "dom")
MESH = pl.DeviceIdType.MESH
f32 = jnp.float32
bf16 = jnp.bfloat16
highest = lax.Precision.HIGHEST
LANES = 128
CHUNKS = 4
ROWS_LHS = 176
TN = (((0,), (0,)), ((), ()))
NT = (((1,), (1,)), ((), ()))


def offset_of(slot):
    return slot + 1 if slot < REACH else REACH - 1 - slot


def split(value):
    hi = value.astype(bf16)
    return hi, (value - hi.astype(f32)).astype(bf16)


def lane_block(number):
    return pl.ds(pl.multiple_of(number * LANES, LANES), LANES)


def make_kernel(groups, places, elems, cap):
    slots = 2 * REACH + 2
    blocks = elems // LANES
    sent = slots * cap
    receivers = 16

    def kernel(
        count_ref, send_count_ref, rec_element_ref, rec_slot_ref,
        state_ref, stiff_ref, flux_ref, fluxr_ref, star_hbm, face_hbm, facer_hbm,
        energy_weight_ref, near_ref, send_ref, rec_weight_ref,
        x_ref, energy_ref, trace_ref,
        star_ref, face_ref, facer_ref, weight_ref, live_ref, recw_ref, names_ref,
        y_ref, v_ref, part_ref, xt_ref, send_buf, halo_ref, hb_ref, own_ref, nb_ref, vr_ref,
        pick_ref, pack_ref, af_ref, a_ref, rf_ref, ra_ref,
        en_ref, rec_ref, table_ref, msg_ref, all_ref,
        send_sem, recv_sem, last_send, last_recv, load_sem,
    ):
        g = lax.axis_index("grp")
        d = lax.axis_index("dom")

        loads = [
            pltpu.make_async_copy(source, held, load_sem.at[i])
            for i, (source, held) in enumerate(
                [(star_hbm, star_ref), (face_hbm, face_ref), (facer_hbm, facer_ref)]
            )
        ]
        for load in loads:
            load.start()

        for t in range(STEPS):
            halo_ref[t, 2 * REACH * cap :, :] = jnp.zeros((2 * cap, CHUNKS * LANES), f32)
        barrier = pltpu.get_barrier_semaphore()

        def greet(k, carry):
            peer = lax.rem(d + k, places)
            pl.semaphore_signal(barrier, inc=1, device_id=(g, peer), device_id_type=MESH)
            return carry

        lax.fori_loop(1, places, greet, 0)

        @pl.when(g < groups - 1)
        def _():
            pl.semaphore_signal(barrier, inc=1, device_id=(g + 1, d), device_id_type=MESH)

        @pl.when(g > 0)
        def _():
            pl.semaphore_signal(barrier, inc=1, device_id=(g - 1, d), device_id_type=MESH)

        for q in range(9):
            x_ref[q] = state_ref[q]
        here = lax.broadcasted_iota(jnp.int32, (1, elems), 1)
        live = jnp.clip((count_ref[0] - here).astype(f32), 0.0, 1.0)
        live_ref[...] = live
        for q in range(9):
            weight_ref[q] = energy_weight_ref[q : q + 1, :] * live

        lane = lax.broadcasted_iota(jnp.int32, (LANES, LANES), 1).astype(f32)

        def hot(names, tile):
            return jnp.maximum(1.0 - jnp.abs(names - (lane[: names.shape[0]] + float(tile * LANES))), 0.0).astype(bf16)

        names_ref[...] = jnp.zeros_like(names_ref)
        names_ref[0:slots, 0:cap] = send_ref[0].astype(f32)
        turned = names_ref[...].T
        order = lax.broadcasted_iota(jnp.int32, (cap, LANES), 0)
        for slot in range(slots):
            sends = jnp.clip((send_count_ref[0, slot] - order).astype(f32), 0.0, 1.0)
            names = (jnp.broadcast_to(turned[:cap, slot : slot + 1], (cap, LANES)) + 1.0) * sends - 1.0
            for tile in range(blocks):
                pack_ref[slot * cap : (slot + 1) * cap, tile * LANES : (tile + 1) * LANES] = hot(names, tile)

        def listed(ref):
            rows = lax.broadcasted_iota(jnp.int32, (receivers, LANES), 0)
            total = jnp.zeros((receivers, LANES), f32)
            for r in range(receivers):
                total = total + jnp.where(rows == r, 1.0, 0.0) * ref[r].astype(f32)
            return total

        names = listed(rec_element_ref)
        for tile in range(blocks):
            pack_ref[sent : sent + receivers, tile * LANES : (tile + 1) * LANES] = hot(names, tile)

        def to_rows():
            def body(block, carry):
                at = lane_block(block)
                for j in range(CHUNKS):
                    size = min(16, 56 - 16 * j)
                    pieces = [x_ref[2 * j, :, at], x_ref[2 * j + 1, :, at], x_ref[8, pl.ds(16 * j, size), at]]
                    if size < 16:
                        pieces.append(jnp.zeros((16 - size, LANES), f32))
                    hi, lo = split(jnp.concatenate(pieces, axis=0).T)
                    xt_ref[at, 2 * j * LANES : (2 * j + 1) * LANES] = hi
                    xt_ref[at, (2 * j + 1) * LANES : (2 * j + 2) * LANES] = lo
                return carry

            lax.fori_loop(0, blocks, body, 0)

        def pack(first, count):
            for j in range(CHUNKS):
                taken = jnp.dot(
                    pack_ref[first : first + count, :],
                    xt_ref[:, 2 * j * LANES : (2 * j + 2) * LANES],
                    preferred_element_type=f32,
                )
                whole = taken[:, :LANES] + taken[:, LANES:]
                if first == 0:
                    send_buf[:, j * LANES : (j + 1) * LANES] = whole[:sent]
                    rec_ref[:, j * LANES : (j + 1) * LANES] = whole[sent:]
                else:
                    rec_ref[:, j * LANES : (j + 1) * LANES] = whole

        def copies(t):
            made = []
            for slot in range(slots):
                if slot < 2 * REACH:
                    target = (g, lax.rem(d + offset_of(slot) + places, places))
                else:
                    target = (g + (1 if slot == 2 * REACH else -1), d)
                made.append(
                    pltpu.make_async_remote_copy(
                        src_ref=send_buf.at[pl.ds(slot * cap, cap)],
                        dst_ref=halo_ref.at[t, pl.ds(slot * cap, cap)],
                        send_sem=send_sem.at[slot],
                        recv_sem=recv_sem.at[t, slot],
                        device_id=target,
                        device_id_type=MESH,
                    )
                )
            return made

        def trace(t):
            at = lax.broadcasted_iota(jnp.int32, (CHUNKS * LANES, LANES), 0)
            inside = at % LANES
            quantity = jnp.where(inside < 56, at // LANES * 2, jnp.where(inside < 112, at // LANES * 2 + 1, 8))
            out = lax.broadcasted_iota(jnp.int32, (CHUNKS * LANES, LANES), 1)
            placed = jnp.where(out == 9 * t + quantity, 1.0, 0.0).astype(f32)
            table_ref[...] += jnp.dot(
                rec_ref[...] * recw_ref[...], placed, precision=highest, preferred_element_type=f32
            )

        to_rows()
        table_ref[...] = jnp.zeros_like(table_ref)
        en_ref[...] = jnp.zeros_like(en_ref)

        def step(t, carry):
            pack(0, sent + receivers)

            @pl.when(t == 0)
            def _():
                waits = places - 1 + jnp.where(g > 0, 1, 0) + jnp.where(g < groups - 1, 1, 0)
                pl.semaphore_wait(barrier, waits)

            moves = copies(t)
            for slot in range(2 * REACH):
                moves[slot].start()

            @pl.when(g < groups - 1)
            def _():
                moves[6].start()

            @pl.when(g > 0)
            def _():
                moves[7].start()

            @pl.when(t == 0)
            def _():
                af_ref[...] = jnp.zeros_like(af_ref)
                for m in range(7):
                    matrix = stiff_ref[m] if m < 3 else -flux_ref[m - 3]
                    for part in range(4):
                        af_ref[pl.ds(56 * m, 56), pl.ds(64 * part, 56)] = matrix
                whole = af_ref[...]
                rounded = whole.astype(bf16).astype(f32)
                part = lax.broadcasted_iota(jnp.int32, whole.shape, 1) // 64
                a_ref[...] = jnp.where(part % 2 == 0, rounded, whole - rounded).astype(bf16)
                for f in range(4):
                    matrix = -fluxr_ref[f]
                    for j in range(CHUNKS):
                        rf_ref[...] = jnp.zeros_like(rf_ref)
                        rf_ref[pl.ds(0, 56), pl.ds(0, 56)] = matrix
                        rf_ref[pl.ds(56, 56), pl.ds(56, 56)] = matrix
                        size = min(16, 56 - 16 * j)
                        rf_ref[pl.ds(112, 56), pl.ds(112, size)] = matrix[:, 16 * j : 16 * j + size]
                        hi, lo = split(rf_ref[...])
                        ra_ref[f, j, :ROWS_LHS] = jnp.concatenate([hi, hi], axis=1)
                        ra_ref[f, j, ROWS_LHS:] = jnp.concatenate([lo, lo], axis=1)

                def face_rows(block, carry):
                    at = lane_block(block)
                    for f in range(4):
                        row = near_ref[f : f + 1, at].astype(f32)
                        names = jnp.broadcast_to(row, (LANES, LANES)).T
                        for tile in range(blocks + sent // LANES):
                            pick_ref[f, at, tile * LANES : (tile + 1) * LANES] = hot(names, tile)
                    return carry

                lax.fori_loop(0, blocks, face_rows, 0)
                for j in range(CHUNKS):
                    size = min(16, 56 - 16 * j)
                    recw_ref[:, j * LANES : (j + 1) * LANES] = jnp.zeros((receivers, LANES), f32)
                    recw_ref[:, j * LANES : j * LANES + 56] = rec_weight_ref[...]
                    recw_ref[:, j * LANES + 56 : j * LANES + 112] = rec_weight_ref[...]
                    recw_ref[:, j * LANES + 112 : j * LANES + 112 + size] = rec_weight_ref[:, 16 * j : 16 * j + size]
                for load in loads:
                    load.wait()

            @pl.when(t > 0)
            def _():
                trace(t - 1)

            def modal(q, carry):
                pad = jnp.zeros((8, elems), f32)
                value = jnp.concatenate([x_ref[q], pad], axis=0)
                hi, lo = split(value)
                y_ref[0:64, :] = hi
                y_ref[64:128, :] = hi
                y_ref[128:192, :] = lo
                y_ref[192:256, :] = lo
                v_ref[q] = jnp.dot(a_ref[...], y_ref[...], preferred_element_type=f32)
                return carry

            lax.fori_loop(0, 9, modal, 0)

            def local_map(number, carry):
                block = number // 3
                first = (number % 3) * 3
                at = lane_block(block)
                total = [jnp.zeros((56, LANES), f32) for _ in range(3)]
                for m in range(7):
                    maps, n = (star_ref, m) if m < 3 else (face_ref, m - 3)
                    for q in range(9):
                        term = v_ref[q, pl.ds(56 * m, 56), at]
                        for i in range(3):
                            total[i] = total[i] + maps[first + i, q, pl.ds(n, 1), at] * term
                for i in range(3):
                    part_ref[first + i, :, at] = total[i]
                return carry

            lax.fori_loop(0, blocks * 3, local_map, 0)

            def own(f, carry):
                for j in range(CHUNKS):
                    own_ref[f, j] = jnp.dot(
                        pick_ref[f, :, :elems],
                        xt_ref[:, 2 * j * LANES : (2 * j + 2) * LANES],
                        preferred_element_type=f32,
                    ).astype(bf16)
                return carry

            lax.fori_loop(0, 4, own, 0)

            for slot in range(2 * REACH):
                moves[slot].wait_recv()

            @pl.when(g > 0)
            def _():
                moves[6].wait_recv()

            @pl.when(g < groups - 1)
            def _():
                moves[7].wait_recv()

            for j in range(CHUNKS):
                hi, lo = split(halo_ref[t, :, j * LANES : (j + 1) * LANES])
                hb_ref[:, 2 * j * LANES : (2 * j + 1) * LANES] = hi
                hb_ref[:, (2 * j + 1) * LANES : (2 * j + 2) * LANES] = lo

            def remote(f, carry):
                for j in range(CHUNKS):
                    far = jnp.dot(
                        pick_ref[f, :, elems:],
                        hb_ref[:, 2 * j * LANES : (2 * j + 2) * LANES],
                        preferred_element_type=f32,
                    ).astype(bf16)
                    nb_ref[...] = own_ref[f, j] + far
                    near = nb_ref[...]
                    both = lax.dot_general(ra_ref[f, j], near, NT, preferred_element_type=f32)
                    both = both[:ROWS_LHS] + both[ROWS_LHS:]
                    vr_ref[f, 2 * j] = both[0:56]
                    vr_ref[f, 2 * j + 1] = both[56:112]
                    if j == 0:
                        vr_ref[f, 8] = both[112:168]
                    else:
                        vr_ref[f, 8] += both[112:168]
                return carry

            lax.fori_loop(0, 4, remote, 0)

            def remote_map(number, energy):
                block = number // 3
                first = (number % 3) * 3
                at = lane_block(block)
                live = live_ref[:, at]
                total = [part_ref[first + i, :, at] for i in range(3)]
                for f in range(4):
                    for q in range(9):
                        term = vr_ref[f, q, :, at]
                        for i in range(3):
                            total[i] = total[i] + facer_ref[first + i, q, pl.ds(f, 1), at] * term
                for i in range(3):
                    new = x_ref[first + i, :, at] + live * total[i]
                    x_ref[first + i, :, at] = new
                    squares = jnp.sum(new * new, axis=0, keepdims=True)
                    energy = energy + weight_ref[first + i, :, at] * squares
                return energy

            energy = lax.fori_loop(0, blocks * 3, remote_map, jnp.zeros((1, LANES), f32))
            sub = lax.broadcasted_iota(jnp.int32, (8, LANES), 0)
            en_ref[...] += jnp.where(sub == t, energy, 0.0)
            to_rows()

            for slot in range(2 * REACH):
                moves[slot].wait_send()

            @pl.when(g < groups - 1)
            def _():
                moves[6].wait_send()

            @pl.when(g > 0)
            def _():
                moves[7].wait_send()

            return carry

        lax.fori_loop(0, STEPS, step, 0)
        pack(sent, receivers)
        trace(STEPS - 1)

        row = lax.broadcasted_iota(jnp.int32, (receivers, LANES), 0)
        col = lax.broadcasted_iota(jnp.int32, (receivers, LANES), 1)
        rows = listed(rec_slot_ref)
        sums = jnp.sum(en_ref[...], axis=1, keepdims=True)
        table = table_ref[...] + jnp.where(col == 27, rows, 0.0)
        for t in range(STEPS):
            table = table + jnp.where((col == 28 + t) & (row == 0), sums[t : t + 1], 0.0)
        half = receivers // 2
        msg_ref[...] = table[:half] + pltpu.roll(table[half:], 64, 1)

        def last(k):
            return pltpu.make_async_remote_copy(
                src_ref=msg_ref,
                dst_ref=all_ref.at[d],
                send_sem=last_send.at[k],
                recv_sem=last_recv.at[k],
                device_id=(g, lax.rem(d + k, places)),
                device_id_type=MESH,
            )

        def arrival(k):
            return pltpu.make_async_remote_copy(
                src_ref=msg_ref,
                dst_ref=all_ref.at[lax.rem(d + places - k, places)],
                send_sem=last_send.at[k],
                recv_sem=last_recv.at[k],
                device_id=(g, lax.rem(d + k, places)),
                device_id_type=MESH,
            )

        def start_last(k, carry):
            last(k).start()
            return carry

        def end_last(k, carry):
            arrival(k).wait_recv()
            last(k).wait_send()
            return carry

        lax.fori_loop(1, places, start_last, 0)
        all_ref[d] = msg_ref[...]
        lax.fori_loop(1, places, end_last, 0)

        arrived = all_ref[...].reshape(places * half, LANES)
        summed = jnp.sum(arrived, axis=0, keepdims=True)
        energy_ref[...] = summed[:, 28 : 28 + STEPS] * (0.5 / float(places * elems * 56 * 9))
        mine = lax.broadcasted_iota(jnp.int32, (places * half, LANES), 1).astype(f32)
        mine = mine + (d * receivers).astype(f32)
        keep = lax.broadcasted_iota(jnp.int32, (places * half, LANES), 1) < receivers
        result = jnp.zeros((32, LANES), f32)
        for part in range(2):
            names = jnp.broadcast_to(arrived[:, 64 * part + 27 : 64 * part + 28], (places * half, LANES))
            chosen = jnp.maximum(1.0 - jnp.abs(names - mine), 0.0)
            chosen = jnp.where(keep, chosen, 0.0)
            picked = lax.dot_general(arrived, chosen, TN, precision=highest, preferred_element_type=f32)
            result = result + picked[64 * part : 64 * part + 32]
        for t in range(STEPS):
            for q in range(9):
                trace_ref[q, t : t + 1, :] = result[9 * t + q : 9 * t + q + 1, :receivers]

    return kernel


def per_device(groups, places):
    def run(
        element_state, stiffness, flux_local, flux_remote, star_matrix, face_local, face_remote,
        energy_weight, face_neighbour, element_count, send_count, send_element,
        receiver_element, receiver_slot, receiver_weight,
    ):
        basis, quantities, elems = element_state.shape
        slots, cap = send_element.shape[1:]
        sent = slots * cap
        receivers = receiver_slot.shape[0]
        vmem = pl.BlockSpec(memory_space=pltpu.VMEM)
        smem = pl.BlockSpec(memory_space=pltpu.SMEM)
        hbm = pl.BlockSpec(memory_space=pl.ANY)
        wide = CHUNKS * LANES
        faces = 4
        state, energy, traces = pl.pallas_call(
            make_kernel(groups, places, elems, cap),
            out_shape=(
                jax.ShapeDtypeStruct((quantities, basis, elems), f32),
                jax.ShapeDtypeStruct((1, STEPS), f32),
                jax.ShapeDtypeStruct((quantities, STEPS, receivers), f32),
            ),
            in_specs=[smem] * 4 + [vmem] * 4 + [hbm] * 3 + [vmem] * 4,
            out_specs=(vmem, vmem, vmem),
            scratch_shapes=[
                pltpu.VMEM((9, 9, 3, elems), f32),
                pltpu.VMEM((9, 9, faces, elems), f32),
                pltpu.VMEM((9, 9, faces, elems), f32),
                pltpu.VMEM((9, 1, elems), f32),
                pltpu.VMEM((1, elems), f32),
                pltpu.VMEM((receivers, wide), f32),
                pltpu.VMEM((LANES, LANES), f32),
                pltpu.VMEM((256, elems), bf16),
                pltpu.VMEM((9, 400, elems), f32),
                pltpu.VMEM((9, 56, elems), f32),
                pltpu.VMEM((elems, 2 * wide), bf16),
                pltpu.VMEM((sent, wide), f32),
                pltpu.VMEM((STEPS, sent, wide), f32),
                pltpu.VMEM((sent, 2 * wide), bf16),
                pltpu.VMEM((faces, CHUNKS, elems, 2 * LANES), bf16),
                pltpu.VMEM((elems, 2 * LANES), bf16),
                pltpu.VMEM((faces, 9, 56, elems), f32),
                pltpu.VMEM((faces, elems, elems + sent), bf16),
                pltpu.VMEM((sent + LANES, elems), bf16),
                pltpu.VMEM((400, 256), f32),
                pltpu.VMEM((400, 256), bf16),
                pltpu.VMEM((ROWS_LHS, LANES), f32),
                pltpu.VMEM((faces, CHUNKS, 2 * ROWS_LHS, 2 * LANES), bf16),
                pltpu.VMEM((8, LANES), f32),
                pltpu.VMEM((receivers, wide), f32),
                pltpu.VMEM((receivers, LANES), f32),
                pltpu.VMEM((receivers // 2, LANES), f32),
                pltpu.VMEM((places, receivers // 2, LANES), f32),
                pltpu.SemaphoreType.DMA((slots,)),
                pltpu.SemaphoreType.DMA((STEPS, slots)),
                pltpu.SemaphoreType.DMA((places,)),
                pltpu.SemaphoreType.DMA((places,)),
                pltpu.SemaphoreType.DMA((3,)),
            ],
            compiler_params=pltpu.CompilerParams(
                collective_id=0, has_side_effects=True, vmem_limit_bytes=60 * 1024 * 1024
            ),
        )(
            element_count, send_count, receiver_element, receiver_slot,
            element_state.transpose(1, 0, 2), stiffness, flux_local, flux_remote,
            star_matrix.transpose(1, 2, 0, 3), face_local.transpose(1, 2, 0, 3),
            face_remote.transpose(1, 2, 0, 3),
            energy_weight, face_neighbour, send_element, receiver_weight.T,
        )
        return state.transpose(1, 0, 2), energy, traces.transpose(1, 0, 2)

    return run


def solution(mesh):
    return jax.shard_map(
        per_device(mesh.shape["grp"], mesh.shape["dom"]),
        mesh=mesh,
        in_specs=(
            P(None, None, GRP_DOM), P(), P(), P(),
            P(None, None, None, GRP_DOM), P(None, None, None, GRP_DOM), P(None, None, None, GRP_DOM),
            P(None, GRP_DOM), P(None, GRP_DOM), P(GRP_DOM), P(GRP_DOM, None), P(GRP_DOM, None, None),
            P(GRP_DOM), P(GRP_DOM), P(None, GRP_DOM),
        ),
        out_specs=(P(None, None, GRP_DOM), P("grp", None), P(None, None, GRP_DOM)),
        check_vma=False,
    )
```

```python
import jax
import jax.numpy as jnp
from jax import lax
from jax.experimental import pallas as pl
from jax.experimental.pallas import tpu as pltpu
from jax.sharding import PartitionSpec as P

STEPS = 3
REACH = 3
GRP_DOM = ("grp", "dom")
MESH = pl.DeviceIdType.MESH
f32 = jnp.float32
bf16 = jnp.bfloat16
highest = lax.Precision.HIGHEST
LANES = 128
CHUNKS = 4
ROWS_LHS = 176
TN = (((0,), (0,)), ((), ()))
NT = (((1,), (1,)), ((), ()))


def offset_of(slot):
    return slot + 1 if slot < REACH else REACH - 1 - slot


def split(value):
    hi = value.astype(bf16)
    return hi, (value - hi.astype(f32)).astype(bf16)


def lane_block(number):
    return pl.ds(pl.multiple_of(number * LANES, LANES), LANES)


def make_kernel(groups, places, elems, cap):
    slots = 2 * REACH + 2
    blocks = elems // LANES
    sent = slots * cap
    receivers = 16

    def kernel(
        count_ref, send_count_ref, rec_element_ref, rec_slot_ref,
        state_ref, stiff_ref, flux_ref, fluxr_ref, star_hbm, face_hbm, facer_hbm,
        energy_weight_ref, near_ref, send_ref, rec_weight_ref,
        x_ref, energy_ref, trace_ref,
        star_ref, face_ref, facer_ref, weight_ref, live_ref, recw_ref, names_ref,
        y_ref, v_ref, part_ref, xt_ref, send_buf, halo_ref, hb_ref, own_ref, nb_ref, vra_ref, vrb_ref,
        pick_ref, pack_ref, af_ref, a_ref, rf_ref, ra_ref,
        en_ref, rec_ref, table_ref, msg_ref, all_ref,
        send_sem, recv_sem, last_send, last_recv, load_sem,
    ):
        g = lax.axis_index("grp")
        d = lax.axis_index("dom")

        loads = [
            pltpu.make_async_copy(source, held, load_sem.at[i])
            for i, (source, held) in enumerate(
                [(star_hbm, star_ref), (face_hbm, face_ref), (facer_hbm, facer_ref)]
            )
        ]
        for load in loads:
            load.start()

        for t in range(STEPS):
            halo_ref[t, 2 * REACH * cap :, :] = jnp.zeros((2 * cap, CHUNKS * LANES), f32)
        barrier = pltpu.get_barrier_semaphore()

        def greet(k, carry):
            peer = lax.rem(d + k, places)
            pl.semaphore_signal(barrier, inc=1, device_id=(g, peer), device_id_type=MESH)
            return carry

        lax.fori_loop(1, places, greet, 0)

        @pl.when(g < groups - 1)
        def _():
            pl.semaphore_signal(barrier, inc=1, device_id=(g + 1, d), device_id_type=MESH)

        @pl.when(g > 0)
        def _():
            pl.semaphore_signal(barrier, inc=1, device_id=(g - 1, d), device_id_type=MESH)

        for q in range(9):
            x_ref[q] = state_ref[q]
        here = lax.broadcasted_iota(jnp.int32, (1, elems), 1)
        live = jnp.clip((count_ref[0] - here).astype(f32), 0.0, 1.0)
        live_ref[...] = live
        for q in range(9):
            weight_ref[q] = energy_weight_ref[q : q + 1, :] * live

        lane = lax.broadcasted_iota(jnp.int32, (LANES, LANES), 1).astype(f32)

        def hot(names, tile):
            return jnp.maximum(1.0 - jnp.abs(names - (lane[: names.shape[0]] + float(tile * LANES))), 0.0).astype(bf16)

        names_ref[...] = jnp.zeros_like(names_ref)
        names_ref[0:slots, 0:cap] = send_ref[0].astype(f32)
        turned = names_ref[...].T
        order = lax.broadcasted_iota(jnp.int32, (cap, LANES), 0)
        for slot in range(slots):
            sends = jnp.clip((send_count_ref[0, slot] - order).astype(f32), 0.0, 1.0)
            names = (jnp.broadcast_to(turned[:cap, slot : slot + 1], (cap, LANES)) + 1.0) * sends - 1.0
            for tile in range(blocks):
                pack_ref[slot * cap : (slot + 1) * cap, tile * LANES : (tile + 1) * LANES] = hot(names, tile)

        def listed(ref):
            rows = lax.broadcasted_iota(jnp.int32, (receivers, LANES), 0)
            total = jnp.zeros((receivers, LANES), f32)
            for r in range(receivers):
                total = total + jnp.where(rows == r, 1.0, 0.0) * ref[r].astype(f32)
            return total

        names = listed(rec_element_ref)
        for tile in range(blocks):
            pack_ref[sent : sent + receivers, tile * LANES : (tile + 1) * LANES] = hot(names, tile)

        def to_rows():
            def body(block, carry):
                at = lane_block(block)
                for j in range(CHUNKS):
                    size = min(16, 56 - 16 * j)
                    pieces = [x_ref[2 * j, :, at], x_ref[2 * j + 1, :, at], x_ref[8, pl.ds(16 * j, size), at]]
                    if size < 16:
                        pieces.append(jnp.zeros((16 - size, LANES), f32))
                    hi, lo = split(jnp.concatenate(pieces, axis=0).T)
                    xt_ref[at, 2 * j * LANES : (2 * j + 1) * LANES] = hi
                    xt_ref[at, (2 * j + 1) * LANES : (2 * j + 2) * LANES] = lo
                return carry

            lax.fori_loop(0, blocks, body, 0)

        def pack(first, count):
            for j in range(CHUNKS):
                taken = jnp.dot(
                    pack_ref[first : first + count, :],
                    xt_ref[:, 2 * j * LANES : (2 * j + 2) * LANES],
                    preferred_element_type=f32,
                )
                whole = taken[:, :LANES] + taken[:, LANES:]
                if first == 0:
                    send_buf[:, j * LANES : (j + 1) * LANES] = whole[:sent]
                    rec_ref[:, j * LANES : (j + 1) * LANES] = whole[sent:]
                else:
                    rec_ref[:, j * LANES : (j + 1) * LANES] = whole

        def copies(t):
            made = []
            for slot in range(slots):
                if slot < 2 * REACH:
                    target = (g, lax.rem(d + offset_of(slot) + places, places))
                else:
                    target = (g + (1 if slot == 2 * REACH else -1), d)
                made.append(
                    pltpu.make_async_remote_copy(
                        src_ref=send_buf.at[pl.ds(slot * cap, cap)],
                        dst_ref=halo_ref.at[t, pl.ds(slot * cap, cap)],
                        send_sem=send_sem.at[slot],
                        recv_sem=recv_sem.at[t, slot],
                        device_id=target,
                        device_id_type=MESH,
                    )
                )
            return made

        def trace(t):
            at = lax.broadcasted_iota(jnp.int32, (CHUNKS * LANES, LANES), 0)
            inside = at % LANES
            quantity = jnp.where(inside < 56, at // LANES * 2, jnp.where(inside < 112, at // LANES * 2 + 1, 8))
            out = lax.broadcasted_iota(jnp.int32, (CHUNKS * LANES, LANES), 1)
            placed = jnp.where(out == 9 * t + quantity, 1.0, 0.0).astype(f32)
            table_ref[...] += jnp.dot(
                rec_ref[...] * recw_ref[...], placed, precision=highest, preferred_element_type=f32
            )

        to_rows()
        table_ref[...] = jnp.zeros_like(table_ref)
        en_ref[...] = jnp.zeros_like(en_ref)

        def step(t, carry):
            pack(0, sent + receivers)

            @pl.when(t == 0)
            def _():
                waits = places - 1 + jnp.where(g > 0, 1, 0) + jnp.where(g < groups - 1, 1, 0)
                pl.semaphore_wait(barrier, waits)

            moves = copies(t)
            for slot in range(2 * REACH):
                moves[slot].start()

            @pl.when(g < groups - 1)
            def _():
                moves[6].start()

            @pl.when(g > 0)
            def _():
                moves[7].start()

            @pl.when(t == 0)
            def _():
                af_ref[...] = jnp.zeros_like(af_ref)
                for m in range(7):
                    matrix = stiff_ref[m] if m < 3 else -flux_ref[m - 3]
                    for part in range(4):
                        af_ref[pl.ds(56 * m, 56), pl.ds(64 * part, 56)] = matrix
                whole = af_ref[...]
                rounded = whole.astype(bf16).astype(f32)
                part = lax.broadcasted_iota(jnp.int32, whole.shape, 1) // 64
                a_ref[...] = jnp.where(part % 2 == 0, rounded, whole - rounded).astype(bf16)
                for f in range(4):
                    matrix = -fluxr_ref[f]
                    for j in range(CHUNKS):
                        rf_ref[...] = jnp.zeros_like(rf_ref)
                        rf_ref[pl.ds(0, 56), pl.ds(0, 56)] = matrix
                        rf_ref[pl.ds(56, 56), pl.ds(56, 56)] = matrix
                        size = min(16, 56 - 16 * j)
                        rf_ref[pl.ds(112, 56), pl.ds(112, size)] = matrix[:, 16 * j : 16 * j + size]
                        hi, lo = split(rf_ref[...])
                        ra_ref[f, j, :ROWS_LHS] = jnp.concatenate([hi, hi], axis=1)
                        ra_ref[f, j, ROWS_LHS:] = jnp.concatenate([lo, lo], axis=1)

                def face_rows(block, carry):
                    at = lane_block(block)
                    for f in range(4):
                        row = near_ref[f : f + 1, at].astype(f32)
                        names = jnp.broadcast_to(row, (LANES, LANES)).T
                        for tile in range(blocks + sent // LANES):
                            pick_ref[f, at, tile * LANES : (tile + 1) * LANES] = hot(names, tile)
                    return carry

                lax.fori_loop(0, blocks, face_rows, 0)
                for j in range(CHUNKS):
                    size = min(16, 56 - 16 * j)
                    recw_ref[:, j * LANES : (j + 1) * LANES] = jnp.zeros((receivers, LANES), f32)
                    recw_ref[:, j * LANES : j * LANES + 56] = rec_weight_ref[...]
                    recw_ref[:, j * LANES + 56 : j * LANES + 112] = rec_weight_ref[...]
                    recw_ref[:, j * LANES + 112 : j * LANES + 112 + size] = rec_weight_ref[:, 16 * j : 16 * j + size]
                for load in loads:
                    load.wait()

            @pl.when(t > 0)
            def _():
                trace(t - 1)

            def modal(q, carry):
                pad = jnp.zeros((8, elems), f32)
                value = jnp.concatenate([x_ref[q], pad], axis=0)
                hi, lo = split(value)
                y_ref[0:64, :] = hi
                y_ref[64:128, :] = hi
                y_ref[128:192, :] = lo
                y_ref[192:256, :] = lo
                v_ref[q] = jnp.dot(a_ref[...], y_ref[...], preferred_element_type=f32)
                return carry

            lax.fori_loop(0, 9, modal, 0)

            def local_map(number, carry):
                block = number // 3
                first = (number % 3) * 3
                at = lane_block(block)
                total = [jnp.zeros((56, LANES), f32) for _ in range(3)]
                for m in range(7):
                    maps, n = (star_ref, m) if m < 3 else (face_ref, m - 3)
                    for q in range(9):
                        term = v_ref[q, pl.ds(56 * m, 56), at]
                        for i in range(3):
                            total[i] = total[i] + maps[first + i, q, pl.ds(n, 1), at] * term
                for i in range(3):
                    part_ref[first + i, :, at] = total[i]
                own(number)
                return carry

            def own(unit):
                f, j = unit // CHUNKS, unit % CHUNKS
                pair = pl.ds(pl.multiple_of(j * 2 * LANES, 2 * LANES), 2 * LANES)
                own_ref[f, j] = jnp.dot(
                    pick_ref[f, :, :elems], xt_ref[:, pair], preferred_element_type=f32
                ).astype(bf16)

            lax.fori_loop(0, blocks * 3, local_map, 0)
            for unit in range(blocks * 3, 4 * CHUNKS):
                own(unit)

            for slot in range(2 * REACH):
                moves[slot].wait_recv()

            @pl.when(g > 0)
            def _():
                moves[6].wait_recv()

            @pl.when(g < groups - 1)
            def _():
                moves[7].wait_recv()

            for j in range(CHUNKS):
                hi, lo = split(halo_ref[t, :, j * LANES : (j + 1) * LANES])
                hb_ref[:, 2 * j * LANES : (2 * j + 1) * LANES] = hi
                hb_ref[:, (2 * j + 1) * LANES : (2 * j + 2) * LANES] = lo

            def far_unit(f, j, held):
                far = jnp.dot(
                    pick_ref[f, :, elems:],
                    hb_ref[:, 2 * j * LANES : (2 * j + 2) * LANES],
                    preferred_element_type=f32,
                ).astype(bf16)
                nb_ref[...] = own_ref[f, j] + far
                both = lax.dot_general(ra_ref[f, j], nb_ref[...], NT, preferred_element_type=f32)
                both = both[:ROWS_LHS] + both[ROWS_LHS:]
                held[2 * j] = both[0:56]
                held[2 * j + 1] = both[56:112]
                if j == 0:
                    held[8] = both[112:168]
                else:
                    held[8] += both[112:168]

            def face_map(f, held, block, first):
                at = pl.ds(block * LANES, LANES)
                total = [part_ref[first + i, :, at] for i in range(3)]
                for q in range(9):
                    term = held[q, :, at]
                    for i in range(3):
                        total[i] = total[i] + facer_ref[first + i, q, f : f + 1, at] * term
                for i in range(3):
                    part_ref[first + i, :, at] = total[i]

            held = [vra_ref, vrb_ref]
            units = [(block, 3 * i) for block in range(blocks) for i in range(3)]
            for f in range(4):

                @pl.when(t < STEPS + f)
                def _():
                    for j in range(CHUNKS):
                        far_unit(f, j, held[f % 2])
                        if f > 0:
                            for block, first in units[j::CHUNKS]:
                                face_map(f - 1, held[(f - 1) % 2], block, first)

            def remote_map(number, energy):
                block = number // 3
                first = (number % 3) * 3
                at = lane_block(block)
                live = live_ref[:, at]
                total = [part_ref[first + i, :, at] for i in range(3)]
                for q in range(9):
                    term = vrb_ref[q, :, at]
                    for i in range(3):
                        total[i] = total[i] + facer_ref[first + i, q, pl.ds(3, 1), at] * term
                for i in range(3):
                    new = x_ref[first + i, :, at] + live * total[i]
                    x_ref[first + i, :, at] = new
                    squares = jnp.sum(new * new, axis=0, keepdims=True)
                    energy = energy + weight_ref[first + i, :, at] * squares
                return energy

            energy = lax.fori_loop(0, blocks * 3, remote_map, jnp.zeros((1, LANES), f32))
            sub = lax.broadcasted_iota(jnp.int32, (8, LANES), 0)
            en_ref[...] += jnp.where(sub == t, energy, 0.0)
            to_rows()

            for slot in range(2 * REACH):
                moves[slot].wait_send()

            @pl.when(g < groups - 1)
            def _():
                moves[6].wait_send()

            @pl.when(g > 0)
            def _():
                moves[7].wait_send()

            return carry

        lax.fori_loop(0, STEPS, step, 0)
        pack(sent, receivers)
        trace(STEPS - 1)

        row = lax.broadcasted_iota(jnp.int32, (receivers, LANES), 0)
        col = lax.broadcasted_iota(jnp.int32, (receivers, LANES), 1)
        rows = listed(rec_slot_ref)
        sums = jnp.sum(en_ref[...], axis=1, keepdims=True)
        table = table_ref[...] + jnp.where(col == 27, rows, 0.0)
        for t in range(STEPS):
            table = table + jnp.where((col == 28 + t) & (row == 0), sums[t : t + 1], 0.0)
        half = receivers // 2
        msg_ref[...] = table[:half] + pltpu.roll(table[half:], 64, 1)

        def last(k):
            return pltpu.make_async_remote_copy(
                src_ref=msg_ref,
                dst_ref=all_ref.at[d],
                send_sem=last_send.at[k],
                recv_sem=last_recv.at[k],
                device_id=(g, lax.rem(d + k, places)),
                device_id_type=MESH,
            )

        def arrival(k):
            return pltpu.make_async_remote_copy(
                src_ref=msg_ref,
                dst_ref=all_ref.at[lax.rem(d + places - k, places)],
                send_sem=last_send.at[k],
                recv_sem=last_recv.at[k],
                device_id=(g, lax.rem(d + k, places)),
                device_id_type=MESH,
            )

        def start_last(k, carry):
            last(k).start()
            return carry

        def end_last(k, carry):
            arrival(k).wait_recv()
            last(k).wait_send()
            return carry

        lax.fori_loop(1, places, start_last, 0)
        all_ref[d] = msg_ref[...]
        lax.fori_loop(1, places, end_last, 0)

        arrived = all_ref[...].reshape(places * half, LANES)
        summed = jnp.sum(arrived, axis=0, keepdims=True)
        energy_ref[...] = summed[:, 28 : 28 + STEPS] * (0.5 / float(places * elems * 56 * 9))
        mine = lax.broadcasted_iota(jnp.int32, (places * half, LANES), 1).astype(f32)
        mine = mine + (d * receivers).astype(f32)
        keep = lax.broadcasted_iota(jnp.int32, (places * half, LANES), 1) < receivers
        result = jnp.zeros((32, LANES), f32)
        for part in range(2):
            names = jnp.broadcast_to(arrived[:, 64 * part + 27 : 64 * part + 28], (places * half, LANES))
            chosen = jnp.maximum(1.0 - jnp.abs(names - mine), 0.0)
            chosen = jnp.where(keep, chosen, 0.0)
            picked = lax.dot_general(arrived, chosen, TN, precision=highest, preferred_element_type=f32)
            result = result + picked[64 * part : 64 * part + 32]
        for t in range(STEPS):
            for q in range(9):
                trace_ref[q, t : t + 1, :] = result[9 * t + q : 9 * t + q + 1, :receivers]

    return kernel


def per_device(groups, places):
    def run(
        element_state, stiffness, flux_local, flux_remote, star_matrix, face_local, face_remote,
        energy_weight, face_neighbour, element_count, send_count, send_element,
        receiver_element, receiver_slot, receiver_weight,
    ):
        basis, quantities, elems = element_state.shape
        slots, cap = send_element.shape[1:]
        sent = slots * cap
        receivers = receiver_slot.shape[0]
        vmem = pl.BlockSpec(memory_space=pltpu.VMEM)
        smem = pl.BlockSpec(memory_space=pltpu.SMEM)
        hbm = pl.BlockSpec(memory_space=pl.ANY)
        wide = CHUNKS * LANES
        faces = 4
        state, energy, traces = pl.pallas_call(
            make_kernel(groups, places, elems, cap),
            out_shape=(
                jax.ShapeDtypeStruct((quantities, basis, elems), f32),
                jax.ShapeDtypeStruct((1, STEPS), f32),
                jax.ShapeDtypeStruct((quantities, STEPS, receivers), f32),
            ),
            in_specs=[smem] * 4 + [vmem] * 4 + [hbm] * 3 + [vmem] * 4,
            out_specs=(vmem, vmem, vmem),
            scratch_shapes=[
                pltpu.VMEM((9, 9, 3, elems), f32),
                pltpu.VMEM((9, 9, faces, elems), f32),
                pltpu.VMEM((9, 9, faces, elems), f32),
                pltpu.VMEM((9, 1, elems), f32),
                pltpu.VMEM((1, elems), f32),
                pltpu.VMEM((receivers, wide), f32),
                pltpu.VMEM((LANES, LANES), f32),
                pltpu.VMEM((256, elems), bf16),
                pltpu.VMEM((9, 400, elems), f32),
                pltpu.VMEM((9, 56, elems), f32),
                pltpu.VMEM((elems, 2 * wide), bf16),
                pltpu.VMEM((sent, wide), f32),
                pltpu.VMEM((STEPS, sent, wide), f32),
                pltpu.VMEM((sent, 2 * wide), bf16),
                pltpu.VMEM((faces, CHUNKS, elems, 2 * LANES), bf16),
                pltpu.VMEM((elems, 2 * LANES), bf16),
                pltpu.VMEM((9, 56, elems), f32),
                pltpu.VMEM((9, 56, elems), f32),
                pltpu.VMEM((faces, elems, elems + sent), bf16),
                pltpu.VMEM((sent + LANES, elems), bf16),
                pltpu.VMEM((400, 256), f32),
                pltpu.VMEM((400, 256), bf16),
                pltpu.VMEM((ROWS_LHS, LANES), f32),
                pltpu.VMEM((faces, CHUNKS, 2 * ROWS_LHS, 2 * LANES), bf16),
                pltpu.VMEM((8, LANES), f32),
                pltpu.VMEM((receivers, wide), f32),
                pltpu.VMEM((receivers, LANES), f32),
                pltpu.VMEM((receivers // 2, LANES), f32),
                pltpu.VMEM((places, receivers // 2, LANES), f32),
                pltpu.SemaphoreType.DMA((slots,)),
                pltpu.SemaphoreType.DMA((STEPS, slots)),
                pltpu.SemaphoreType.DMA((places,)),
                pltpu.SemaphoreType.DMA((places,)),
                pltpu.SemaphoreType.DMA((3,)),
            ],
            compiler_params=pltpu.CompilerParams(
                collective_id=0, has_side_effects=True, vmem_limit_bytes=60 * 1024 * 1024
            ),
        )(
            element_count, send_count, receiver_element, receiver_slot,
            element_state.transpose(1, 0, 2), stiffness, flux_local, flux_remote,
            star_matrix.transpose(1, 2, 0, 3), face_local.transpose(1, 2, 0, 3),
            face_remote.transpose(1, 2, 0, 3),
            energy_weight, face_neighbour, send_element, receiver_weight.T,
        )
        return state.transpose(1, 0, 2), energy, traces.transpose(1, 0, 2)

    return run


def solution(mesh):
    return jax.shard_map(
        per_device(mesh.shape["grp"], mesh.shape["dom"]),
        mesh=mesh,
        in_specs=(
            P(None, None, GRP_DOM), P(), P(), P(),
            P(None, None, None, GRP_DOM), P(None, None, None, GRP_DOM), P(None, None, None, GRP_DOM),
            P(None, GRP_DOM), P(None, GRP_DOM), P(GRP_DOM), P(GRP_DOM, None), P(GRP_DOM, None, None),
            P(GRP_DOM), P(GRP_DOM), P(None, GRP_DOM),
        ),
        out_specs=(P(None, None, GRP_DOM), P("grp", None), P(None, None, GRP_DOM)),
        check_vma=False,
    )
```

```python
import jax
import jax.numpy as jnp
from jax import lax
from jax.experimental import pallas as pl
from jax.experimental.pallas import tpu as pltpu
from jax.sharding import PartitionSpec as P

STEPS = 3
REACH = 3
GRP_DOM = ("grp", "dom")
MESH = pl.DeviceIdType.MESH
f32 = jnp.float32
bf16 = jnp.bfloat16
highest = lax.Precision.HIGHEST
LANES = 128
CHUNKS = 4
ROWS_LHS = 176
TN = (((0,), (0,)), ((), ()))
NT = (((1,), (1,)), ((), ()))


def offset_of(slot):
    return slot + 1 if slot < REACH else REACH - 1 - slot


def split(value):
    hi = value.astype(bf16)
    return hi, (value - hi.astype(f32)).astype(bf16)


def lane_block(number):
    return pl.ds(pl.multiple_of(number * LANES, LANES), LANES)


def make_kernel(groups, places, elems, cap):
    slots = 2 * REACH + 2
    blocks = elems // LANES
    sent = slots * cap
    receivers = 16

    def kernel(
        count_ref, send_count_ref, rec_element_ref, rec_slot_ref,
        state_ref, stiff_ref, flux_ref, fluxr_ref, star_hbm, face_hbm, facer_hbm,
        energy_weight_ref, near_ref, send_ref, rec_weight_ref,
        x_ref, energy_ref, trace_ref,
        star_ref, face_ref, facer_ref, weight_ref, live_ref, recw_ref, names_ref,
        y_ref, v_ref, part_ref, xt_ref, send_buf, halo_ref, hb_ref, own_ref, nb_ref, vra_ref, vrb_ref,
        pick_ref, pack_ref, af_ref, a_ref, rf_ref, ra_ref,
        en_ref, rec_ref, table_ref, msg_ref, all_ref,
        send_sem, recv_sem, last_send, last_recv, load_sem,
    ):
        g = lax.axis_index("grp")
        d = lax.axis_index("dom")

        loads = [
            pltpu.make_async_copy(source, held, load_sem.at[i])
            for i, (source, held) in enumerate(
                [(star_hbm, star_ref), (face_hbm, face_ref), (facer_hbm, facer_ref)]
            )
        ]
        for load in loads:
            load.start()

        for t in range(STEPS):
            halo_ref[t, 2 * REACH * cap :, :] = jnp.zeros((2 * cap, CHUNKS * LANES), f32)
        barrier = pltpu.get_barrier_semaphore()

        def greet(k, carry):
            peer = lax.rem(d + k, places)
            pl.semaphore_signal(barrier, inc=1, device_id=(g, peer), device_id_type=MESH)
            return carry

        lax.fori_loop(1, places, greet, 0)

        @pl.when(g < groups - 1)
        def _():
            pl.semaphore_signal(barrier, inc=1, device_id=(g + 1, d), device_id_type=MESH)

        @pl.when(g > 0)
        def _():
            pl.semaphore_signal(barrier, inc=1, device_id=(g - 1, d), device_id_type=MESH)

        for q in range(9):
            x_ref[q] = state_ref[q]
        here = lax.broadcasted_iota(jnp.int32, (1, elems), 1)
        live = jnp.clip((count_ref[0] - here).astype(f32), 0.0, 1.0)
        live_ref[...] = live
        for q in range(9):
            weight_ref[q] = energy_weight_ref[q : q + 1, :] * live

        lane = lax.broadcasted_iota(jnp.int32, (LANES, LANES), 1).astype(f32)

        def hot(away, tile):
            step = (away - float(tile * LANES)).astype(bf16)
            return jnp.maximum(1.0 - step * step, 0.0)

        names_ref[...] = jnp.zeros_like(names_ref)
        names_ref[0:slots, 0:cap] = send_ref[0].astype(f32)
        turned = names_ref[...].T
        order = lax.broadcasted_iota(jnp.int32, (cap, LANES), 0)
        for slot in range(slots):
            sends = jnp.clip((send_count_ref[0, slot] - order).astype(f32), 0.0, 1.0)
            names = (jnp.broadcast_to(turned[:cap, slot : slot + 1], (cap, LANES)) + 1.0) * sends - 1.0
            away = names - lane[:cap]
            for tile in range(blocks):
                pack_ref[slot * cap : (slot + 1) * cap, tile * LANES : (tile + 1) * LANES] = hot(away, tile)

        def listed(ref):
            rows = lax.broadcasted_iota(jnp.int32, (receivers, LANES), 0)
            total = jnp.zeros((receivers, LANES), f32)
            for r in range(receivers):
                total = total + jnp.where(rows == r, 1.0, 0.0) * ref[r].astype(f32)
            return total

        away = listed(rec_element_ref) - lane[:receivers]
        for tile in range(blocks):
            pack_ref[sent : sent + receivers, tile * LANES : (tile + 1) * LANES] = hot(away, tile)

        def to_rows():
            def body(block, carry):
                at = lane_block(block)
                for j in range(CHUNKS):
                    size = min(16, 56 - 16 * j)
                    pieces = [x_ref[2 * j, :, at], x_ref[2 * j + 1, :, at], x_ref[8, pl.ds(16 * j, size), at]]
                    if size < 16:
                        pieces.append(jnp.zeros((16 - size, LANES), f32))
                    hi, lo = split(jnp.concatenate(pieces, axis=0).T)
                    xt_ref[at, 2 * j * LANES : (2 * j + 1) * LANES] = hi
                    xt_ref[at, (2 * j + 1) * LANES : (2 * j + 2) * LANES] = lo
                return carry

            lax.fori_loop(0, blocks, body, 0)

        def pack(first, count):
            for j in range(CHUNKS):
                taken = jnp.dot(
                    pack_ref[first : first + count, :],
                    xt_ref[:, 2 * j * LANES : (2 * j + 2) * LANES],
                    preferred_element_type=f32,
                )
                whole = taken[:, :LANES] + taken[:, LANES:]
                if first == 0:
                    send_buf[:, j * LANES : (j + 1) * LANES] = whole[:sent]
                    rec_ref[:, j * LANES : (j + 1) * LANES] = whole[sent:]
                else:
                    rec_ref[:, j * LANES : (j + 1) * LANES] = whole

        def copies(t):
            made = []
            for slot in range(slots):
                if slot < 2 * REACH:
                    target = (g, lax.rem(d + offset_of(slot) + places, places))
                else:
                    target = (g + (1 if slot == 2 * REACH else -1), d)
                made.append(
                    pltpu.make_async_remote_copy(
                        src_ref=send_buf.at[pl.ds(slot * cap, cap)],
                        dst_ref=halo_ref.at[t, pl.ds(slot * cap, cap)],
                        send_sem=send_sem.at[slot],
                        recv_sem=recv_sem.at[t, slot],
                        device_id=target,
                        device_id_type=MESH,
                    )
                )
            return made

        def trace(t):
            at = lax.broadcasted_iota(jnp.int32, (CHUNKS * LANES, LANES), 0)
            inside = at % LANES
            quantity = jnp.where(inside < 56, at // LANES * 2, jnp.where(inside < 112, at // LANES * 2 + 1, 8))
            out = lax.broadcasted_iota(jnp.int32, (CHUNKS * LANES, LANES), 1)
            placed = jnp.where(out == 9 * t + quantity, 1.0, 0.0).astype(f32)
            table_ref[...] += jnp.dot(
                rec_ref[...] * recw_ref[...], placed, precision=highest, preferred_element_type=f32
            )

        to_rows()
        table_ref[...] = jnp.zeros_like(table_ref)
        en_ref[...] = jnp.zeros_like(en_ref)

        def step(t, carry):
            pack(0, sent + receivers)

            @pl.when(t == 0)
            def _():
                waits = places - 1 + jnp.where(g > 0, 1, 0) + jnp.where(g < groups - 1, 1, 0)
                pl.semaphore_wait(barrier, waits)

            moves = copies(t)
            for slot in range(2 * REACH):
                moves[slot].start()

            @pl.when(g < groups - 1)
            def _():
                moves[6].start()

            @pl.when(g > 0)
            def _():
                moves[7].start()

            @pl.when(t == 0)
            def _():
                af_ref[...] = jnp.zeros_like(af_ref)
                for m in range(7):
                    matrix = stiff_ref[m] if m < 3 else -flux_ref[m - 3]
                    for part in range(4):
                        af_ref[pl.ds(56 * m, 56), pl.ds(64 * part, 56)] = matrix
                whole = af_ref[...]
                rounded = whole.astype(bf16).astype(f32)
                part = lax.broadcasted_iota(jnp.int32, whole.shape, 1) // 64
                a_ref[...] = jnp.where(part % 2 == 0, rounded, whole - rounded).astype(bf16)
                for f in range(4):
                    matrix = -fluxr_ref[f]
                    for j in range(CHUNKS):
                        rf_ref[...] = jnp.zeros_like(rf_ref)
                        rf_ref[pl.ds(0, 56), pl.ds(0, 56)] = matrix
                        rf_ref[pl.ds(56, 56), pl.ds(56, 56)] = matrix
                        size = min(16, 56 - 16 * j)
                        rf_ref[pl.ds(112, 56), pl.ds(112, size)] = matrix[:, 16 * j : 16 * j + size]
                        hi, lo = split(rf_ref[...])
                        ra_ref[f, j, :ROWS_LHS] = jnp.concatenate([hi, hi], axis=1)
                        ra_ref[f, j, ROWS_LHS:] = jnp.concatenate([lo, lo], axis=1)

                def face_rows(block, carry):
                    at = lane_block(block)
                    for f in range(4):
                        row = near_ref[f : f + 1, at].astype(f32)
                        away = jnp.broadcast_to(row, (LANES, LANES)).T - lane
                        for tile in range(blocks + sent // LANES):
                            pick_ref[f, at, tile * LANES : (tile + 1) * LANES] = hot(away, tile)
                    return carry

                lax.fori_loop(0, blocks, face_rows, 0)
                for j in range(CHUNKS):
                    size = min(16, 56 - 16 * j)
                    recw_ref[:, j * LANES : (j + 1) * LANES] = jnp.zeros((receivers, LANES), f32)
                    recw_ref[:, j * LANES : j * LANES + 56] = rec_weight_ref[...]
                    recw_ref[:, j * LANES + 56 : j * LANES + 112] = rec_weight_ref[...]
                    recw_ref[:, j * LANES + 112 : j * LANES + 112 + size] = rec_weight_ref[:, 16 * j : 16 * j + size]
                for load in loads:
                    load.wait()

            @pl.when(t > 0)
            def _():
                trace(t - 1)

            def modal(q, carry):
                pad = jnp.zeros((8, elems), f32)
                value = jnp.concatenate([x_ref[q], pad], axis=0)
                hi, lo = split(value)
                y_ref[0:64, :] = hi
                y_ref[64:128, :] = hi
                y_ref[128:192, :] = lo
                y_ref[192:256, :] = lo
                v_ref[q] = jnp.dot(a_ref[...], y_ref[...], preferred_element_type=f32)
                return carry

            lax.fori_loop(0, 9, modal, 0)

            def local_map(number, carry):
                block = number // 3
                first = (number % 3) * 3
                at = lane_block(block)
                total = [jnp.zeros((56, LANES), f32) for _ in range(3)]
                for m in range(7):
                    maps, n = (star_ref, m) if m < 3 else (face_ref, m - 3)
                    for q in range(9):
                        term = v_ref[q, pl.ds(56 * m, 56), at]
                        for i in range(3):
                            total[i] = total[i] + maps[first + i, q, pl.ds(n, 1), at] * term
                for i in range(3):
                    part_ref[first + i, :, at] = total[i]
                own(number)
                return carry

            def own(unit):
                f, j = unit // CHUNKS, unit % CHUNKS
                pair = pl.ds(pl.multiple_of(j * 2 * LANES, 2 * LANES), 2 * LANES)
                own_ref[f, j] = jnp.dot(
                    pick_ref[f, :, :elems], xt_ref[:, pair], preferred_element_type=f32
                ).astype(bf16)

            lax.fori_loop(0, blocks * 3, local_map, 0)
            for unit in range(blocks * 3, 4 * CHUNKS):
                own(unit)

            for slot in range(2 * REACH):
                moves[slot].wait_recv()

            @pl.when(g > 0)
            def _():
                moves[6].wait_recv()

            @pl.when(g < groups - 1)
            def _():
                moves[7].wait_recv()

            for j in range(CHUNKS):
                hi, lo = split(halo_ref[t, :, j * LANES : (j + 1) * LANES])
                hb_ref[:, 2 * j * LANES : (2 * j + 1) * LANES] = hi
                hb_ref[:, (2 * j + 1) * LANES : (2 * j + 2) * LANES] = lo

            def far_unit(f, j, held):
                far = jnp.dot(
                    pick_ref[f, :, elems:],
                    hb_ref[:, 2 * j * LANES : (2 * j + 2) * LANES],
                    preferred_element_type=f32,
                ).astype(bf16)
                nb_ref[...] = own_ref[f, j] + far
                both = lax.dot_general(ra_ref[f, j], nb_ref[...], NT, preferred_element_type=f32)
                both = both[:ROWS_LHS] + both[ROWS_LHS:]
                held[2 * j] = both[0:56]
                held[2 * j + 1] = both[56:112]
                if j == 0:
                    held[8] = both[112:168]
                else:
                    held[8] += both[112:168]

            def face_map(f, held, block, first):
                at = pl.ds(block * LANES, LANES)
                total = [part_ref[first + i, :, at] for i in range(3)]
                for q in range(9):
                    term = held[q, :, at]
                    for i in range(3):
                        total[i] = total[i] + facer_ref[first + i, q, f : f + 1, at] * term
                for i in range(3):
                    part_ref[first + i, :, at] = total[i]

            held = [vra_ref, vrb_ref]
            units = [(block, 3 * i) for block in range(blocks) for i in range(3)]
            for f in range(4):

                @pl.when(t < STEPS + f)
                def _():
                    for j in range(CHUNKS):
                        far_unit(f, j, held[f % 2])
                        if f > 0:
                            for block, first in units[j::CHUNKS]:
                                face_map(f - 1, held[(f - 1) % 2], block, first)

            def remote_map(number, energy):
                block = number // 3
                first = (number % 3) * 3
                at = lane_block(block)
                live = live_ref[:, at]
                total = [part_ref[first + i, :, at] for i in range(3)]
                for q in range(9):
                    term = vrb_ref[q, :, at]
                    for i in range(3):
                        total[i] = total[i] + facer_ref[first + i, q, pl.ds(3, 1), at] * term
                for i in range(3):
                    new = x_ref[first + i, :, at] + live * total[i]
                    x_ref[first + i, :, at] = new
                    squares = jnp.sum(new * new, axis=0, keepdims=True)
                    energy = energy + weight_ref[first + i, :, at] * squares
                return energy

            energy = lax.fori_loop(0, blocks * 3, remote_map, jnp.zeros((1, LANES), f32))
            sub = lax.broadcasted_iota(jnp.int32, (8, LANES), 0)
            en_ref[...] += jnp.where(sub == t, energy, 0.0)
            to_rows()

            for slot in range(2 * REACH):
                moves[slot].wait_send()

            @pl.when(g < groups - 1)
            def _():
                moves[6].wait_send()

            @pl.when(g > 0)
            def _():
                moves[7].wait_send()

            return carry

        lax.fori_loop(0, STEPS, step, 0)
        pack(sent, receivers)
        trace(STEPS - 1)

        row = lax.broadcasted_iota(jnp.int32, (receivers, LANES), 0)
        col = lax.broadcasted_iota(jnp.int32, (receivers, LANES), 1)
        rows = listed(rec_slot_ref)
        sums = jnp.sum(en_ref[...], axis=1, keepdims=True)
        table = table_ref[...] + jnp.where(col == 27, rows, 0.0)
        for t in range(STEPS):
            table = table + jnp.where((col == 28 + t) & (row == 0), sums[t : t + 1], 0.0)
        half = receivers // 2
        msg_ref[...] = table[:half] + pltpu.roll(table[half:], 64, 1)

        def last(k):
            return pltpu.make_async_remote_copy(
                src_ref=msg_ref,
                dst_ref=all_ref.at[d],
                send_sem=last_send.at[k],
                recv_sem=last_recv.at[k],
                device_id=(g, lax.rem(d + k, places)),
                device_id_type=MESH,
            )

        def arrival(k):
            return pltpu.make_async_remote_copy(
                src_ref=msg_ref,
                dst_ref=all_ref.at[lax.rem(d + places - k, places)],
                send_sem=last_send.at[k],
                recv_sem=last_recv.at[k],
                device_id=(g, lax.rem(d + k, places)),
                device_id_type=MESH,
            )

        def start_last(k, carry):
            last(k).start()
            return carry

        def end_last(k, carry):
            arrival(k).wait_recv()
            last(k).wait_send()
            return carry

        lax.fori_loop(1, places, start_last, 0)
        all_ref[d] = msg_ref[...]
        lax.fori_loop(1, places, end_last, 0)

        arrived = all_ref[...].reshape(places * half, LANES)
        summed = jnp.sum(arrived, axis=0, keepdims=True)
        energy_ref[...] = summed[:, 28 : 28 + STEPS] * (0.5 / float(places * elems * 56 * 9))
        mine = lax.broadcasted_iota(jnp.int32, (places * half, LANES), 1).astype(f32)
        mine = mine + (d * receivers).astype(f32)
        keep = lax.broadcasted_iota(jnp.int32, (places * half, LANES), 1) < receivers
        result = jnp.zeros((32, LANES), f32)
        for part in range(2):
            names = jnp.broadcast_to(arrived[:, 64 * part + 27 : 64 * part + 28], (places * half, LANES))
            chosen = jnp.maximum(1.0 - jnp.abs(names - mine), 0.0)
            chosen = jnp.where(keep, chosen, 0.0)
            picked = lax.dot_general(arrived, chosen, TN, precision=highest, preferred_element_type=f32)
            result = result + picked[64 * part : 64 * part + 32]
        for t in range(STEPS):
            for q in range(9):
                trace_ref[q, t : t + 1, :] = result[9 * t + q : 9 * t + q + 1, :receivers]

    return kernel


def per_device(groups, places):
    def run(
        element_state, stiffness, flux_local, flux_remote, star_matrix, face_local, face_remote,
        energy_weight, face_neighbour, element_count, send_count, send_element,
        receiver_element, receiver_slot, receiver_weight,
    ):
        basis, quantities, elems = element_state.shape
        slots, cap = send_element.shape[1:]
        sent = slots * cap
        receivers = receiver_slot.shape[0]
        vmem = pl.BlockSpec(memory_space=pltpu.VMEM)
        smem = pl.BlockSpec(memory_space=pltpu.SMEM)
        hbm = pl.BlockSpec(memory_space=pl.ANY)
        wide = CHUNKS * LANES
        faces = 4
        state, energy, traces = pl.pallas_call(
            make_kernel(groups, places, elems, cap),
            out_shape=(
                jax.ShapeDtypeStruct((quantities, basis, elems), f32),
                jax.ShapeDtypeStruct((1, STEPS), f32),
                jax.ShapeDtypeStruct((quantities, STEPS, receivers), f32),
            ),
            in_specs=[smem] * 4 + [vmem] * 4 + [hbm] * 3 + [vmem] * 4,
            out_specs=(vmem, vmem, vmem),
            scratch_shapes=[
                pltpu.VMEM((9, 9, 3, elems), f32),
                pltpu.VMEM((9, 9, faces, elems), f32),
                pltpu.VMEM((9, 9, faces, elems), f32),
                pltpu.VMEM((9, 1, elems), f32),
                pltpu.VMEM((1, elems), f32),
                pltpu.VMEM((receivers, wide), f32),
                pltpu.VMEM((LANES, LANES), f32),
                pltpu.VMEM((256, elems), bf16),
                pltpu.VMEM((9, 400, elems), f32),
                pltpu.VMEM((9, 56, elems), f32),
                pltpu.VMEM((elems, 2 * wide), bf16),
                pltpu.VMEM((sent, wide), f32),
                pltpu.VMEM((STEPS, sent, wide), f32),
                pltpu.VMEM((sent, 2 * wide), bf16),
                pltpu.VMEM((faces, CHUNKS, elems, 2 * LANES), bf16),
                pltpu.VMEM((elems, 2 * LANES), bf16),
                pltpu.VMEM((9, 56, elems), f32),
                pltpu.VMEM((9, 56, elems), f32),
                pltpu.VMEM((faces, elems, elems + sent), bf16),
                pltpu.VMEM((sent + LANES, elems), bf16),
                pltpu.VMEM((400, 256), f32),
                pltpu.VMEM((400, 256), bf16),
                pltpu.VMEM((ROWS_LHS, LANES), f32),
                pltpu.VMEM((faces, CHUNKS, 2 * ROWS_LHS, 2 * LANES), bf16),
                pltpu.VMEM((8, LANES), f32),
                pltpu.VMEM((receivers, wide), f32),
                pltpu.VMEM((receivers, LANES), f32),
                pltpu.VMEM((receivers // 2, LANES), f32),
                pltpu.VMEM((places, receivers // 2, LANES), f32),
                pltpu.SemaphoreType.DMA((slots,)),
                pltpu.SemaphoreType.DMA((STEPS, slots)),
                pltpu.SemaphoreType.DMA((places,)),
                pltpu.SemaphoreType.DMA((places,)),
                pltpu.SemaphoreType.DMA((3,)),
            ],
            compiler_params=pltpu.CompilerParams(
                collective_id=0, has_side_effects=True, vmem_limit_bytes=60 * 1024 * 1024
            ),
        )(
            element_count, send_count, receiver_element, receiver_slot,
            element_state.transpose(1, 0, 2), stiffness, flux_local, flux_remote,
            star_matrix.transpose(1, 2, 0, 3), face_local.transpose(1, 2, 0, 3),
            face_remote.transpose(1, 2, 0, 3),
            energy_weight, face_neighbour, send_element, receiver_weight.T,
        )
        return state.transpose(1, 0, 2), energy, traces.transpose(1, 0, 2)

    return run


def solution(mesh):
    return jax.shard_map(
        per_device(mesh.shape["grp"], mesh.shape["dom"]),
        mesh=mesh,
        in_specs=(
            P(None, None, GRP_DOM), P(), P(), P(),
            P(None, None, None, GRP_DOM), P(None, None, None, GRP_DOM), P(None, None, None, GRP_DOM),
            P(None, GRP_DOM), P(None, GRP_DOM), P(GRP_DOM), P(GRP_DOM, None), P(GRP_DOM, None, None),
            P(GRP_DOM), P(GRP_DOM), P(None, GRP_DOM),
        ),
        out_specs=(P(None, None, GRP_DOM), P("grp", None), P(None, None, GRP_DOM)),
        check_vma=False,
    )
```
